128 devices in a mesh: client: 32 (over z, x, core), head: 4 (over y).
Axes of the slice: x: 4, y: 4, z: 4, core: 2. Of those that a mesh axis runs over, the one named last changes fastest.
Arguments:
- pre: bfloat16 [40960, 4096], P('client'), may hold values from -40 to 40
- delta: float32 [40960, 4096], P('client', 'head'), may hold values from -300 to 300
- head_weight: bfloat16 [4096, 4096], P(None, 'head'), may hold values from -0.09375 to 0.09375
- client_ids: int32 [512], P('client'), may hold values from 0 to 511, as said below
Outputs:
- head_grad: float32 [4096, 4096], P('client', 'head')
- bias_grad: float32 [4096], P('head')
- embed_grad: float32 [512, 4096], P('client', 'head')
- span_grad: float32 [80, 4096], P(None, 'head')
The draws below stay inside these ranges and needn't reach their ends.
Inputs may be any that keep to these rules, and one draw needn't show every extreme that they name: `client_ids`: each of the 512 clients appears exactly once.
All inputs are finite; a program needn't handle non-finite values.
Results may differ from the reference program's by a relative error of at most 0.024.
Values may be sent and summed in bfloat16 or wider, within the bound.
No kernel may reach another device: no remote copies, remote signals or barrier semaphores. Data moves between devices by JAX's collectives and lax.ppermute only.
A program may use at most 128 MiB of HBM per device.

```python
import jax
import jax.numpy as jnp
from jax import lax

HID = 4096
EMIT = 4096
SPANS = 80
CLIENTS = 512
ROWS = 40960
N_HEAD = 4


def shuffled_clients(key):
    return jax.random.permutation(jax.random.fold_in(key, 31), CLIENTS).astype(jnp.int32)


def draw_client_ids(key, part):
    return shuffled_clients(key)


def draw_pre(key, part):
    key_base = jax.random.fold_in(key, 11)
    key_level = jax.random.fold_in(key, 12)
    levels = jax.random.uniform(key_level, (HID,), jnp.float32, 0.0, 0.8)
    levels = levels + 0.48 * jnp.arange(HID, dtype=jnp.float32) / HID
    scales = 0.5 * 10.0 ** levels
    base = jnp.clip(jax.random.normal(key_base, (ROWS, HID), jnp.float32), -4.0, 4.0)
    return (base * scales[None, :]).astype(jnp.bfloat16)


def draw_delta(key, part):
    key_base = jax.random.fold_in(key, 21)
    key_rows = jax.random.fold_in(key, 22)
    key_cols = jax.random.fold_in(key, 23)
    owners = shuffled_clients(key).astype(jnp.float32) / CLIENTS
    col_levels = jax.random.uniform(key_cols, (EMIT,), jnp.float32, 0.0, 0.5)
    row_levels = jnp.repeat(owners, SPANS, total_repeat_length=ROWS)
    row_levels = row_levels + jax.random.uniform(key_rows, (ROWS,), jnp.float32, 0.0, 0.3)
    base = jnp.clip(jax.random.normal(key_base, (ROWS, EMIT), jnp.float32), -4.0, 4.0)
    values = base * (10.0 ** row_levels)[:, None] * (10.0 ** col_levels)[None, :]
    return values.astype(jnp.float32)


def shard_levels(stream_key, dims, shards, low, high):
    level, own = 1.0, jax.random.fold_in(stream_key, 6)
    for position, blocks in shards:
        heights = jnp.exp(jax.random.uniform(jax.random.fold_in(own, position), (blocks,), jnp.float32, low / len(shards), high / len(shards)))
        level = level * jnp.repeat(heights, dims[position] // blocks).reshape([-1 if axis == position else 1 for axis in range(len(dims))])
    return level


def gaussian(rng, shape, deviation, reach, cuts=(), kind=jnp.bfloat16):
    drawn = jax.random.normal(rng, shape, jnp.float32) * deviation
    if len(cuts) > 0:
        drawn = shard_levels(rng, shape, cuts, -0.22, 0.18) * drawn
    return jnp.clip(drawn, min=-reach, max=reach).astype(kind)


def setup_inputs(seed: int = 0) -> dict:
    key_of = jax.random.split(jax.random.key(seed), 5)
    pre = draw_pre(jax.random.fold_in(key_of[4], 71), 0)
    delta = draw_delta(jax.random.fold_in(key_of[4], 71), 0)
    head_weight = gaussian(key_of[2], (HID, EMIT), HID ** -0.5, 0.09375, ((1, 4),))
    client_ids = draw_client_ids(jax.random.fold_in(key_of[4], 71), 0)
    return {"pre": pre, "delta": delta, "head_weight": head_weight, "client_ids": client_ids}


def silu_slope(values):
    sigma = jax.nn.sigmoid(values)
    return sigma * (1.0 + values * (1.0 - sigma))

def clip_factor(total, number):
    return jnp.minimum(1.0, 1.0 / jnp.sqrt(total / number + 1e-06))

def reference(pre, delta, head_weight, client_ids):
    pre_wide = pre.astype(jnp.float32)
    hidden = jax.nn.silu(pre_wide).astype(jnp.bfloat16)
    delta_low = delta.astype(jnp.bfloat16)
    head_raw = jnp.dot(hidden.T, delta_low, preferred_element_type=jnp.float32)
    bias_raw = lax.optimization_barrier(jnp.sum(delta, axis=0))
    block = EMIT // N_HEAD
    hidden_grad = jnp.zeros((ROWS, HID), jnp.float32)
    for which in range(N_HEAD):
        partial_sum = jnp.dot(delta_low[:, which * block:(which + 1) * block], head_weight[:, which * block:(which + 1) * block].T, preferred_element_type=jnp.float32)
        rounded = lax.optimization_barrier(partial_sum.astype(jnp.bfloat16))
        hidden_grad = hidden_grad + rounded.astype(jnp.float32)
    pre_grad = hidden_grad * silu_slope(pre_wide)
    grouped = pre_grad.reshape(CLIENTS, SPANS, HID)
    client_part = lax.optimization_barrier(jnp.sum(grouped, axis=1))
    span_raw = lax.optimization_barrier(jnp.sum(grouped, axis=0))
    embed_raw = jnp.zeros((CLIENTS, HID), jnp.float32).at[client_ids.astype(jnp.int32)].add(client_part)
    head_factor = clip_factor(jnp.sum(head_raw * head_raw), HID * EMIT)
    embed_factor = clip_factor(jnp.sum(embed_raw * embed_raw), CLIENTS * HID)
    rest_total = jnp.sum(span_raw * span_raw) + jnp.sum(bias_raw * bias_raw)
    rest_factor = clip_factor(rest_total, SPANS * HID + EMIT)
    return (head_factor * head_raw, rest_factor * bias_raw, embed_factor * embed_raw, rest_factor * span_raw)
```

```python
import jax
import jax.numpy as jnp
from jax import lax
from jax.experimental import pallas as pl
from jax.experimental.pallas import tpu as pltpu
from jax.sharding import Mesh
from jax.sharding import PartitionSpec as P

CLIENT = ("client_0", "client_1", "client_2")
EPSILON = 1e-06
LIMIT = 16 * 2**20
LANES = 128

FIRST = ((2, 0), (2, 1), (1, 0), (1, 1), (2, 2), (2, 3), (3, 2), (3, 3))
ALL = tuple((u, v) for u in range(4) for v in range(4))
KEPT = ((3, 0), (3, 1), (0, 0), (0, 1), (1, 2), (1, 3), (0, 2), (0, 3))


def sigmoid(v):
    return 0.5 * jnp.tanh(0.5 * v) + 0.5


def params(limit=LIMIT):
    return pltpu.CompilerParams(dimension_semantics=("arbitrary",), vmem_limit_bytes=limit)


def whole():
    return pl.BlockSpec(memory_space=pltpu.VMEM)


PARTS = 5


def prepare_body(delta, pre, low, turned, sums, units, buffer, arrived, loaded):
    rows = delta.shape[0] // PARTS
    copies = [
        pltpu.make_async_copy(delta.at[pl.ds(k * rows, rows)], buffer.at[k], arrived.at[k]) for k in range(PARTS)
    ]
    for copy in copies:
        copy.start()
    load = pltpu.make_async_copy(pre, units, loaded)
    load.start()
    total = None
    for k in range(PARTS):
        copies[k].wait()
        value = buffer[k]
        narrow = value.astype(jnp.bfloat16)
        low[k * rows : (k + 1) * rows, :] = narrow
        turned[:, k * rows : (k + 1) * rows] = narrow.T
        part = jnp.sum(value.reshape(rows // 8, 8, value.shape[1]), axis=0)
        total = part if total is None else total + part
    sums[...] = total
    load.wait()


def prepare(delta, pre):
    rows, width = delta.shape
    return pl.pallas_call(
        prepare_body,
        in_specs=[pl.BlockSpec(memory_space=pltpu.HBM)] * 2,
        out_specs=[whole()] * 4,
        out_shape=[
            jax.ShapeDtypeStruct((rows, width), jnp.bfloat16),
            jax.ShapeDtypeStruct((width, rows), jnp.bfloat16),
            jax.ShapeDtypeStruct((8, width), jnp.float32),
            jax.ShapeDtypeStruct(pre.shape, pre.dtype),
        ],
        scratch_shapes=[
            pltpu.VMEM((PARTS, rows // PARTS, width), jnp.float32),
            pltpu.SemaphoreType.DMA((PARTS,)),
            pltpu.SemaphoreType.DMA(()),
        ],
        compiler_params=pltpu.CompilerParams(vmem_limit_bytes=44 * 2**20),
        name="prepare",
    )(delta, pre)


STEP = 4
TILE = 512
CHUNK = 320
SPANS = 80


def product(i, owner, pre, turned):
    units = []
    for j in range(STEP):
        at = pl.multiple_of(owner[STEP * i + j] * LANES, LANES)
        v = pre[:, pl.ds(at, LANES)].astype(jnp.float32)
        units.append((v * sigmoid(v)).astype(jnp.bfloat16))
    return jnp.dot(turned[...], jnp.concatenate(units, axis=1), preferred_element_type=jnp.float32)


def head_call(body, owners, operands, outs, out_shape):
    grid = pltpu.PrefetchScalarGridSpec(
        num_scalar_prefetch=1,
        grid=(len(FIRST) // STEP,),
        in_specs=[whole()] * len(operands),
        out_specs=[whole()] * outs if outs > 1 else whole(),
    )
    return pl.pallas_call(
        body, grid_spec=grid, out_shape=out_shape, compiler_params=params()
    )(owners, *operands)


def plain_body(owner, pre, turned, out):
    i = pl.program_id(0)
    acc = product(i, owner, pre, turned)
    for j in range(STEP):
        out[STEP * i + j] = acc[:, j * LANES : (j + 1) * LANES].astype(out.dtype)


def partner_product(owners, pre, turned):
    shape = jax.ShapeDtypeStruct((len(FIRST), turned.shape[0], LANES), jnp.bfloat16)
    return head_call(plain_body, owners, (pre, turned), 1, shape)


def loading_body(owner, pre, turned, source, out, loaded, arrived):
    i = pl.program_id(0)
    copy = pltpu.make_async_copy(source, loaded, arrived)

    @pl.when(i == 0)
    def _():
        copy.start()

    plain_body(owner, pre, turned, out)

    @pl.when(i == pl.num_programs(0) - 1)
    def _():
        copy.wait()


def loading_product(owners, pre, turned, source):
    grid = pltpu.PrefetchScalarGridSpec(
        num_scalar_prefetch=1,
        grid=(len(FIRST) // STEP,),
        in_specs=[whole(), whole(), pl.BlockSpec(memory_space=pltpu.HBM)],
        out_specs=[whole()] * 2,
        scratch_shapes=[pltpu.SemaphoreType.DMA(())],
    )
    return pl.pallas_call(
        loading_body,
        grid_spec=grid,
        out_shape=[
            jax.ShapeDtypeStruct((len(FIRST), turned.shape[0], LANES), jnp.bfloat16),
            jax.ShapeDtypeStruct(source.shape, source.dtype),
        ],
        compiler_params=params(32 * 2**20),
    )(owners, pre, turned, source)


def first_body(owner, pre, turned, arrived, near, far):
    i = pl.program_id(0)
    acc = product(i, owner, pre, turned)

    def store(out, base):
        for j in range(STEP):
            piece = acc[:, j * LANES : (j + 1) * LANES]
            out[j] = (piece + arrived[base + j].astype(jnp.float32)).astype(out.dtype)

    @pl.when(i == 0)
    def _():
        store(near, 0)

    @pl.when(i == 1)
    def _():
        store(far, STEP)


def first_product(owners, pre, turned, arrived):
    shape = jax.ShapeDtypeStruct((STEP, turned.shape[0], LANES), jnp.bfloat16)
    return head_call(first_body, owners, (pre, turned, arrived), 2, [shape, shape])


def kept_body(owner, pre, turned, arrived, near, far, send_a, send_b, keep):
    i = pl.program_id(0)
    acc = product(i, owner, pre, turned)

    def store(side, base, send, at):
        for j in range(STEP):
            piece = acc[:, j * LANES : (j + 1) * LANES]
            total = piece + arrived[base + j].astype(jnp.float32) + side[j].astype(jnp.float32)
            if j < STEP // 2:
                send[j] = total.astype(send.dtype)
            else:
                keep[at + j - STEP // 2] = total.astype(keep.dtype)

    @pl.when(i == 0)
    def _():
        store(near, 0, send_a, 0)

    @pl.when(i == 1)
    def _():
        store(far, STEP, send_b, STEP // 2)


def kept_product(owners, pre, turned, arrived, near, far):
    width = turned.shape[0]
    half = jax.ShapeDtypeStruct((STEP // 2, width, LANES), jnp.bfloat16)
    full = jax.ShapeDtypeStruct((STEP, width, LANES), jnp.float32)
    return head_call(kept_body, owners, (pre, turned, arrived, near, far), 3, [half, half, full])


def slope_body(tile, pre, low, weight, out):
    i = pl.program_id(0)
    rows, width = low.shape
    per = width // TILE
    clients = rows // SPANS
    at = pl.multiple_of(tile[i] * TILE, TILE)
    turned = weight[pl.ds(at, TILE), :].T
    put = pl.ds(pl.multiple_of((i % per) * TILE, TILE), TILE)
    spans = None
    for row in range(0, rows, CHUNK):
        part = jnp.dot(low[row : row + CHUNK, :], turned, preferred_element_type=jnp.float32)
        half = 0.5 * pre[row : row + CHUNK, pl.ds(at, TILE)].astype(jnp.float32)
        t = jnp.tanh(half)
        grad = part * ((1.0 + t) * (1.0 + half * (1.0 - t)))
        grad = grad.reshape(CHUNK // SPANS, SPANS, TILE)
        first = row // SPANS
        out[i // per, first : first + CHUNK // SPANS, put] = (0.5 * jnp.sum(grad, axis=1)).astype(out.dtype)
        some = jnp.sum(grad, axis=0)
        spans = some if spans is None else spans + some
    out[i // per, clients:, put] = (0.5 * spans).astype(out.dtype)


def slope_sums(tiles, pre, low, weight, dtype):
    rows, width = low.shape
    lines = rows // SPANS + SPANS
    grid = pltpu.PrefetchScalarGridSpec(
        num_scalar_prefetch=1,
        grid=(2 * width // TILE,),
        in_specs=[whole()] * 3,
        out_specs=whole(),
    )
    return pl.pallas_call(
        slope_body,
        grid_spec=grid,
        out_shape=jax.ShapeDtypeStruct((2, lines, width), dtype),
        compiler_params=params(),
    )(tiles, pre, low, weight)


def small_body(owner, kept, got, got_two, selector, bias, send, keep, square, lines):
    f32 = jnp.float32
    sums = kept[1] + got[1].astype(f32) + got_two[...].astype(f32)
    width = sums.shape[1]
    across = width // LANES
    clients = selector.shape[1]
    mine = sums[:clients]
    square[...] = jnp.full(square.shape, jnp.sum(mine * mine))
    placed = jnp.dot(selector[...], mine.astype(jnp.bfloat16), preferred_element_type=f32)
    spans = sums[clients:]
    lines[...] = jnp.zeros(lines.shape, f32)
    for r in range(SPANS // 8):
        for c in range(across):
            lines[r * across + c] = spans[8 * r : 8 * r + 8, c * LANES : (c + 1) * LANES]
    bias_row = jnp.sum(bias[...], axis=0, keepdims=True)
    for c in range(across):
        lines[SPANS // 8 * across, c : c + 1, :] = bias_row[:, c * LANES : (c + 1) * LANES]
    groups = clients // 8
    share = send.shape[1] - groups * across
    for k in range(2 * send.shape[0]):
        out = send if k < send.shape[0] else keep
        at = k % send.shape[0]
        for g in range(groups):
            for c in range(across):
                top = k * clients + 8 * g
                block = placed[top : top + 8, c * LANES : (c + 1) * LANES]
                out[at, g * across + c] = block.astype(out.dtype)
        out[at, groups * across :] = lines[pl.ds(share * owner[k], share)].astype(out.dtype)


def small_sends(owners, kept, got, got_two, selector, bias, share):
    width = kept.shape[2]
    across = width // LANES
    count = owners.shape[0] // 2
    tiles = selector.shape[1] // 8 * across + share
    shape = (count, tiles, 8, LANES)
    grid = pltpu.PrefetchScalarGridSpec(
        num_scalar_prefetch=1,
        grid=(1,),
        in_specs=[whole()] * 5,
        out_specs=[whole()] * 3,
        scratch_shapes=[pltpu.VMEM((share * owners.shape[0], 8, LANES), jnp.float32)],
    )
    return pl.pallas_call(
        small_body,
        grid_spec=grid,
        out_shape=[
            jax.ShapeDtypeStruct(shape, jnp.bfloat16),
            jax.ShapeDtypeStruct(shape, jnp.float32),
            jax.ShapeDtypeStruct((8, LANES), jnp.float32),
        ],
        compiler_params=params(),
        name="small_sends",
    )(owners, kept, got, got_two, selector, bias)


def simple_call(body, operands, shapes):
    return pl.pallas_call(
        body,
        in_specs=[whole()] * len(operands),
        out_specs=[whole()] * len(shapes),
        out_shape=shapes,
        compiler_params=pltpu.CompilerParams(vmem_limit_bytes=LIMIT),
    )(*operands)


def core_sum_body(keep, arrived, own, one, two, three):
    total = keep[...] + arrived[...].astype(jnp.float32)
    own[...] = total[0:4]
    for k, out in ((1, one), (2, two), (3, three)):
        out[...] = total[4 * k : 4 * k + 4].astype(out.dtype)


def core_sum(keep, arrived):
    shape = (keep.shape[0] // 4, *keep.shape[1:])
    low = jax.ShapeDtypeStruct(shape, jnp.bfloat16)
    return simple_call(
        core_sum_body, (keep, arrived), [jax.ShapeDtypeStruct(shape, jnp.float32), low, low, low]
    )


def join_body(keep, got_a, got_b, own, in_one, in_two, in_three, head, small, one, two, three):
    f32 = jnp.float32
    lines = own.shape[1]
    for k in range(4):
        side = got_a if k < 2 else got_b
        total = keep[k] + side[k % 2].astype(f32)
        tiles = own[k] + in_one[k].astype(f32) + in_two[k].astype(f32) + in_three[k].astype(f32)
        if k == 0:
            head[...] = total
            small[...] = tiles
        else:
            out = (one, two, three)[k - 1]
            width = total.shape[0]
            out[:width] = total.astype(out.dtype)
            for t in range(lines):
                out[width + 8 * t : width + 8 * t + 8, :] = tiles[t].astype(out.dtype)


def join(keep, got_a, got_b, own, arrived):
    width = keep.shape[1]
    lines = own.shape[1]
    low = jax.ShapeDtypeStruct((width + 8 * lines, LANES), jnp.bfloat16)
    return simple_call(
        join_body,
        (keep, got_a, got_b, own, *arrived),
        [
            jax.ShapeDtypeStruct((width, LANES), jnp.float32),
            jax.ShapeDtypeStruct((lines, 8, LANES), jnp.float32),
            low,
            low,
            low,
        ],
    )


def close_body(head, small, square, one, two, three, out, embed, message):
    f32 = jnp.float32
    width = head.shape[0]
    lines = small.shape[0]
    across = width // LANES
    total = head[...]
    for side in (one, two, three):
        total = total + side[:width].astype(f32)
    out[...] = total.T
    share = message.shape[1] - 1
    rows = lines - share
    part = jnp.zeros((8, LANES), f32)
    for t in range(lines):
        at = slice(width + 8 * t, width + 8 * t + 8)
        tile = small[t] + one[at].astype(f32) + two[at].astype(f32) + three[at].astype(f32)
        if t < rows:
            r, c = divmod(t, across)
            embed[8 * r : 8 * r + 8, c * LANES : (c + 1) * LANES] = tile
        else:
            low = tile.astype(message.dtype)
            wide_again = low.astype(f32)
            part = part + wide_again * wide_again
            for p in range(message.shape[0]):
                message[p, t - rows] = low
    head_square = jnp.sum(total * total)
    small_square = jnp.sum(part)
    column = lax.broadcasted_iota(jnp.int32, (8, LANES), 1)
    values = jnp.where(column == 0, head_square, jnp.where(column == 1, square[...], small_square))
    coarse = values.astype(message.dtype)
    fine = (values - coarse.astype(f32)).astype(message.dtype)
    line = lax.broadcasted_iota(jnp.int32, (8, LANES), 0)
    mixed = jnp.where(line == 0, coarse.astype(f32), fine.astype(f32)).astype(message.dtype)
    for p in range(message.shape[0]):
        message[p, share] = mixed


def close(head, small, square, arrived, peers, share):
    width = head.shape[0]
    rows = 8 * (small.shape[0] - share) * LANES // width
    return simple_call(
        close_body,
        (head, small, square, *arrived),
        [
            jax.ShapeDtypeStruct((LANES, width), jnp.float32),
            jax.ShapeDtypeStruct((rows, width), jnp.float32),
            jax.ShapeDtypeStruct((peers, share + 1, 8, LANES), jnp.bfloat16),
        ],
    )


def flipped(first, second):
    pairs = []
    for z in range(4):
        for x in range(4):
            pairs.append(((z * 4 + x) * 2, ((z ^ first[0]) * 4 + (x ^ first[1])) * 2))
            pairs.append(((z * 4 + x) * 2 + 1, ((z ^ second[0]) * 4 + (x ^ second[1])) * 2 + 1))
    return pairs


def along_u(x, k):
    return lax.ppermute(x, CLIENT, flipped((0, k), (k, 0)))


def along_v(x, k):
    return lax.ppermute(x, CLIENT, flipped((k, 0), (0, k)))


def to_core(x):
    return lax.ppermute(x, "client_2", [(0, 1), (1, 0)])


def along_head(x, low, high):
    axes = ("client_2", "head")
    pairs = [(h, h ^ low) for h in range(4)] + [(4 + h, 4 + (h ^ high)) for h in range(4)]
    return lax.ppermute(x, axes, pairs)


def wide(x):
    return x.astype(jnp.float32)


def narrow(x):
    return x.astype(jnp.bfloat16)


def clip_factor(total, number):
    return jnp.minimum(1.0, 1.0 / jnp.sqrt(total / number + EPSILON))


def exchange(x, axes):
    return lax.all_to_all(x, axes, 0, 0, tiled=True)


def per_device(pre, delta, head_weight, client_ids):
    _, hidden_width = pre.shape
    emit_here = delta.shape[1]
    clients_here = client_ids.shape[0]
    head_devices = lax.axis_size("head")
    peers = lax.axis_size(CLIENT)
    z, x, core, head = (lax.axis_index(a) for a in (*CLIENT, "head"))

    def owners(side, places):
        u = jnp.array([p[0] for p in places], jnp.int32)
        v = jnp.array([p[1] for p in places], jnp.int32)
        at_z = jnp.where(side == 0, z ^ v, z ^ u)
        at_x = jnp.where(side == 0, x ^ u, x ^ v)
        return ((at_z * 4 + at_x) * 2 + side).astype(jnp.int32)

    def tiles(places):
        per = emit_here // TILE
        return (jnp.stack(places)[:, None] * per + jnp.arange(per)[None, :]).reshape(-1).astype(jnp.int32)

    other = 1 - core
    listed = jnp.concatenate([owners(other, ALL), owners(core, ALL)])
    rows = (listed[:, None] * clients_here + jnp.arange(clients_here)[None, :]).reshape(-1)
    selector = narrow(rows[:, None] == client_ids[None, :])
    share = -(-(SPANS // 8 * (emit_here // LANES) + 1) // peers)

    step_one = jnp.where(core == 0, 1, 3)
    step_two = jnp.where(core == 0, 3, 1)
    places = (
        owners(other, FIRST),
        owners(other, KEPT),
        owners(core, FIRST),
        owners(core, KEPT),
        tiles((head ^ 2, head ^ step_one)),
        tiles((head ^ step_two, head)),
        listed,
        selector,
    )
    delta, *places = lax.optimization_barrier((delta, *places))
    partner_first, partner_kept, own_first, own_kept, tiles_sent, tiles_kept, listed, selector = places

    low, turned, bias_part, pre = prepare(delta, pre)
    part, head_weight = loading_product(partner_first, pre, turned, head_weight)
    arrived_first = to_core(part)
    part = partner_product(partner_kept, pre, turned)
    arrived_kept = to_core(part)
    near, far = first_product(own_first, pre, turned, arrived_first)
    near = along_u(near, 1)
    far = along_u(far, 3)
    sent = slope_sums(tiles_sent, pre, low, head_weight, jnp.bfloat16)
    got = along_head(sent, 1, 3)
    kept = slope_sums(tiles_kept, pre, low, head_weight, jnp.float32)
    message = narrow(kept[0] + wide(got[0]))
    got_two = along_head(message, 3, 1)
    send_a, send_b, keep = kept_product(own_kept, pre, turned, arrived_kept, near, far)
    got_a = along_u(send_a, 3)
    got_b = along_u(send_b, 1)
    small_send, small_keep, embed_square = small_sends(
        listed, kept, got, got_two, selector, bias_part, share
    )
    small_got = to_core(small_send)
    own, one, two, three = core_sum(small_keep, small_got)
    arrived = along_u(two, 2), along_u(one, 1), along_u(three, 3)
    final, small, one, two, three = join(keep, got_a, got_b, own, arrived)
    arrived = along_v(two, 2), along_v(one, 1), along_v(three, 3)
    head_raw, embed_raw, message = close(final, small, embed_square, arrived, peers, share)

    everyone = exchange(message, CLIENT)
    count = SPANS * emit_here // (8 * LANES)
    lines = everyone[:, :share].reshape(-1, 8, LANES)
    spans = lines[:count].reshape(SPANS // 8, emit_here // LANES, 8, LANES)
    span_raw = wide(spans.transpose(0, 2, 1, 3).reshape(SPANS, emit_here))
    bias_raw = wide(lines[count].reshape(emit_here))
    squares = wide(everyone[:, share, :2, :3]).sum(axis=(0, 1))
    squares = exchange(jnp.broadcast_to(squares[None], (head_devices, 3)), "head").sum(axis=0)

    emit_total = emit_here * head_devices
    clients_total = clients_here * peers
    head_factor = clip_factor(squares[0], hidden_width * emit_total)
    embed_factor = clip_factor(squares[1], clients_total * hidden_width)
    rest_factor = clip_factor(squares[2], SPANS * hidden_width + emit_total)
    return (
        head_factor * head_raw,
        rest_factor * bias_raw,
        embed_factor * embed_raw,
        rest_factor * span_raw,
    )


def solution(mesh):
    torus = Mesh(
        mesh.devices.reshape(4, 4, 2, mesh.shape["head"]),
        ("client_0", "client_1", "client_2", "head"),
    )
    return jax.shard_map(
        per_device,
        mesh=torus,
        in_specs=(P(CLIENT, None), P(CLIENT, "head"), P(None, "head"), P(CLIENT)),
        out_specs=(P(CLIENT, "head"), P("head"), P(CLIENT, "head"), P(None, "head")),
        check_vma=False,
    )
```

```python
import jax
import jax.numpy as jnp
from jax import lax
from jax.experimental import pallas as pl
from jax.experimental.pallas import tpu as pltpu
from jax.sharding import Mesh
from jax.sharding import PartitionSpec as P

CLIENT = ("client_0", "client_1", "client_2")
EPSILON = 1e-06
LIMIT = 16 * 2**20
PREPARE_LIMIT = 44 * 2**20
LANES = 128

FIRST = ((2, 0), (2, 1), (1, 0), (1, 1), (2, 2), (2, 3), (3, 2), (3, 3))
ALL = tuple((u, v) for u in range(4) for v in range(4))
KEPT = ((3, 0), (3, 1), (0, 0), (0, 1), (1, 2), (1, 3), (0, 2), (0, 3))


def sigmoid(v):
    return 0.5 * jnp.tanh(0.5 * v) + 0.5


def params(limit=LIMIT):
    return pltpu.CompilerParams(dimension_semantics=("arbitrary",), vmem_limit_bytes=limit)


def whole():
    return pl.BlockSpec(memory_space=pltpu.VMEM)


PARTS = 5
STEP = 4
TILE = 512
CHUNK = 320
SPANS = 80


def position():
    return tuple(lax.axis_index(a) for a in (*CLIENT, "head"))


def owner_at(side, u, v):
    z, x, _, _ = position()
    at_z = jnp.where(side == 0, z ^ v, z ^ u)
    at_x = jnp.where(side == 0, x ^ u, x ^ v)
    return (at_z * 4 + at_x) * 2 + side


def listed(i, places, j):
    early, late = places[j], places[STEP + j]
    return tuple(jnp.where(i == 0, e, l) for e, l in zip(early, late))


def product(owners, pre, turned):
    units = []
    for owner in owners:
        v = pre[:, pl.ds(pl.multiple_of(owner * LANES, LANES), LANES)].astype(jnp.float32)
        units.append((v * sigmoid(v)).astype(jnp.bfloat16))
    return jnp.dot(turned[...], jnp.concatenate(units, axis=1), preferred_element_type=jnp.float32)


def pieces(acc):
    return [acc[:, j * LANES : (j + 1) * LANES] for j in range(STEP)]


def prepare_body(delta, low, turned, sums, buffer, arrived):
    rows = delta.shape[0] // PARTS
    copies = [
        pltpu.make_async_copy(delta.at[pl.ds(k * rows, rows)], buffer.at[k], arrived.at[k]) for k in range(PARTS)
    ]
    for copy in copies:
        copy.start()
    total = None
    for k in range(PARTS):
        copies[k].wait()
        value = buffer[k]
        narrow = value.astype(jnp.bfloat16)
        low[k * rows : (k + 1) * rows, :] = narrow
        turned[:, k * rows : (k + 1) * rows] = narrow.T
        part = jnp.sum(value.reshape(rows // 8, 8, value.shape[1]), axis=0)
        total = part if total is None else total + part
    sums[...] = total


def prepare(delta):
    rows, width = delta.shape
    return pl.pallas_call(
        prepare_body,
        in_specs=[pl.BlockSpec(memory_space=pltpu.HBM)],
        out_specs=[whole()] * 3,
        out_shape=[
            jax.ShapeDtypeStruct((rows, width), jnp.bfloat16),
            jax.ShapeDtypeStruct((width, rows), jnp.bfloat16),
            jax.ShapeDtypeStruct((8, width), jnp.float32),
        ],
        scratch_shapes=[
            pltpu.VMEM((PARTS, rows // PARTS, width), jnp.float32),
            pltpu.SemaphoreType.DMA((PARTS,)),
        ],
        compiler_params=pltpu.CompilerParams(vmem_limit_bytes=PREPARE_LIMIT),
        cost_estimate=pl.CostEstimate(flops=8 * 10**9, bytes_accessed=2 * 10**7, transcendentals=0),
        name="prepare",
    )(delta)


def head_call(body, operands, out_shape):
    return pl.pallas_call(
        body,
        grid=(len(FIRST) // STEP,),
        in_specs=[whole()] * len(operands),
        out_specs=[whole()] * len(out_shape),
        out_shape=out_shape,
        compiler_params=params(),
    )(*operands)


def partner_body(places, pre, turned, out):
    i = pl.program_id(0)
    other = 1 - lax.axis_index("client_2")
    acc = product([owner_at(other, *listed(i, places, j)) for j in range(STEP)], pre, turned)
    for j, piece in enumerate(pieces(acc)):
        out[STEP * i + j] = piece.astype(out.dtype)


def partner_call(places, pre, turned):
    shape = jax.ShapeDtypeStruct((len(FIRST), turned.shape[0], LANES), jnp.bfloat16)
    return head_call(lambda *refs: partner_body(places, *refs), (pre, turned), [shape])[0]


def first_body(pre, turned, arrived, near, far):
    i = pl.program_id(0)
    core = lax.axis_index("client_2")
    acc = product([owner_at(core, *listed(i, FIRST, j)) for j in range(STEP)], pre, turned)

    def store(out, base):
        for j, piece in enumerate(pieces(acc)):
            out[j] = (piece + arrived[base + j].astype(jnp.float32)).astype(out.dtype)

    @pl.when(i == 0)
    def _():
        store(near, 0)

    @pl.when(i == 1)
    def _():
        store(far, STEP)


def first_call(pre, turned, arrived):
    shape = jax.ShapeDtypeStruct((STEP, turned.shape[0], LANES), jnp.bfloat16)
    return head_call(first_body, (pre, turned, arrived), [shape, shape])


def kept_body(pre, turned, arrived, near, far, send_a, send_b, keep):
    i = pl.program_id(0)
    core = lax.axis_index("client_2")
    acc = product([owner_at(core, *listed(i, KEPT, j)) for j in range(STEP)], pre, turned)

    def store(side, base, send, at):
        for j, piece in enumerate(pieces(acc)):
            total = piece + arrived[base + j].astype(jnp.float32) + side[j].astype(jnp.float32)
            if j < STEP // 2:
                send[j] = total.astype(send.dtype)
            else:
                keep[at + j - STEP // 2] = total.astype(keep.dtype)

    @pl.when(i == 0)
    def _():
        store(near, 0, send_a, 0)

    @pl.when(i == 1)
    def _():
        store(far, STEP, send_b, STEP // 2)


def kept_call(pre, turned, arrived, near, far):
    width = turned.shape[0]
    half = jax.ShapeDtypeStruct((STEP // 2, width, LANES), jnp.bfloat16)
    full = jax.ShapeDtypeStruct((STEP, width, LANES), jnp.float32)
    return head_call(kept_body, (pre, turned, arrived, near, far), [half, half, full])


def slope_body(kept, pre, low, weight, out):
    i = pl.program_id(0)
    _, _, core, head = position()
    rows, width = low.shape
    per = width // TILE
    clients = rows // SPANS
    if kept:
        first, second = jnp.where(core == 0, head ^ 3, head ^ 1), head
    else:
        first, second = head ^ 2, jnp.where(core == 0, head ^ 1, head ^ 3)
    at = pl.multiple_of((jnp.where(i < per, first, second) * per + i % per) * TILE, TILE)
    turned = weight[pl.ds(at, TILE), :].T
    put = pl.ds(pl.multiple_of((i % per) * TILE, TILE), TILE)
    spans = None
    for row in range(0, rows, CHUNK):
        part = jnp.dot(low[row : row + CHUNK, :], turned, preferred_element_type=jnp.float32)
        half = 0.5 * pre[row : row + CHUNK, pl.ds(at, TILE)].astype(jnp.float32)
        t = jnp.tanh(half)
        grad = part * ((1.0 + t) * (1.0 + half * (1.0 - t)))
        grad = grad.reshape(CHUNK // SPANS, SPANS, TILE)
        top = row // SPANS
        out[i // per, top : top + CHUNK // SPANS, put] = (0.5 * jnp.sum(grad, axis=1)).astype(out.dtype)
        some = jnp.sum(grad, axis=0)
        spans = some if spans is None else spans + some
    out[i // per, clients:, put] = (0.5 * spans).astype(out.dtype)


def slope_call(kept, pre, low, weight):
    rows, width = low.shape
    return pl.pallas_call(
        lambda *refs: slope_body(kept, *refs),
        grid=(2 * width // TILE,),
        in_specs=[whole()] * 3,
        out_specs=whole(),
        out_shape=jax.ShapeDtypeStruct((2, rows // SPANS + SPANS, width), jnp.float32 if kept else jnp.bfloat16),
        compiler_params=params(),
        name="slope_kept" if kept else "slope_sent",
    )(pre, low, weight)


def small_body(kept, got, got_two, ids, bias, send, keep, square, lines):
    f32 = jnp.float32
    core = lax.axis_index("client_2")
    sums = kept[1] + got[1].astype(f32) + got_two[...].astype(f32)
    width = sums.shape[1]
    across = width // LANES
    clients = ids.shape[1]
    count = 2 * send.shape[0]
    mine = sums[:clients]
    square[...] = jnp.full(square.shape, jnp.sum(mine * mine))
    line = lax.broadcasted_iota(jnp.int32, (count * clients, clients), 0)
    which = line // clients
    side = jnp.where(which < len(ALL), 1 - core, core)
    target = owner_at(side, (which >> 2) & 3, which & 3) * clients + line % clients
    selector = jnp.where(target == ids[...], 1.0, 0.0).astype(jnp.bfloat16)
    placed = jnp.dot(selector, mine.astype(jnp.bfloat16), preferred_element_type=f32)
    spans = sums[clients:]
    lines[...] = jnp.zeros(lines.shape, f32)
    for r in range(SPANS // 8):
        for c in range(across):
            lines[r * across + c] = spans[8 * r : 8 * r + 8, c * LANES : (c + 1) * LANES]
    bias_row = jnp.sum(bias[...], axis=0, keepdims=True)
    for c in range(across):
        lines[SPANS // 8 * across, c : c + 1, :] = bias_row[:, c * LANES : (c + 1) * LANES]
    groups = clients // 8
    share = send.shape[1] - groups * across
    for k in range(count):
        out = send if k < len(ALL) else keep
        at = k % len(ALL)
        for g in range(groups):
            for c in range(across):
                top = k * clients + 8 * g
                block = placed[top : top + 8, c * LANES : (c + 1) * LANES]
                out[at, g * across + c] = block.astype(out.dtype)
        owner = owner_at(1 - core if k < len(ALL) else core, *ALL[at])
        out[at, groups * across :] = lines[pl.ds(share * owner, share)].astype(out.dtype)


def small_sends(kept, got, got_two, ids, bias, share):
    width = kept.shape[2]
    tiles = ids.shape[1] // 8 * (width // LANES) + share
    shape = (len(ALL), tiles, 8, LANES)
    return pl.pallas_call(
        small_body,
        in_specs=[whole()] * 5,
        out_specs=[whole()] * 3,
        out_shape=[
            jax.ShapeDtypeStruct(shape, jnp.bfloat16),
            jax.ShapeDtypeStruct(shape, jnp.float32),
            jax.ShapeDtypeStruct((8, LANES), jnp.float32),
        ],
        scratch_shapes=[pltpu.VMEM((2 * len(ALL) * share, 8, LANES), jnp.float32)],
        compiler_params=pltpu.CompilerParams(vmem_limit_bytes=LIMIT),
        name="small_sends",
    )(kept, got, got_two, ids, bias)


def simple_call(body, operands, shapes):
    return pl.pallas_call(
        body,
        in_specs=[whole()] * len(operands),
        out_specs=[whole()] * len(shapes),
        out_shape=shapes,
        compiler_params=pltpu.CompilerParams(vmem_limit_bytes=LIMIT),
    )(*operands)


def core_sum_body(keep, arrived, own, one, two, three):
    total = keep[...] + arrived[...].astype(jnp.float32)
    own[...] = total[0:4]
    for k, out in ((1, one), (2, two), (3, three)):
        out[...] = total[4 * k : 4 * k + 4].astype(out.dtype)


def core_sum(keep, arrived):
    shape = (keep.shape[0] // 4, *keep.shape[1:])
    low = jax.ShapeDtypeStruct(shape, jnp.bfloat16)
    return simple_call(
        core_sum_body, (keep, arrived), [jax.ShapeDtypeStruct(shape, jnp.float32), low, low, low]
    )


def join_body(keep, got_a, got_b, own, in_one, in_two, in_three, head, small, one, two, three):
    f32 = jnp.float32
    lines = own.shape[1]
    for k in range(4):
        side = got_a if k < 2 else got_b
        total = keep[k] + side[k % 2].astype(f32)
        tiles = own[k] + in_one[k].astype(f32) + in_two[k].astype(f32) + in_three[k].astype(f32)
        if k == 0:
            head[...] = total
            small[...] = tiles
        else:
            out = (one, two, three)[k - 1]
            width = total.shape[0]
            out[:width] = total.astype(out.dtype)
            for t in range(lines):
                out[width + 8 * t : width + 8 * t + 8, :] = tiles[t].astype(out.dtype)


def join(keep, got_a, got_b, own, arrived):
    width = keep.shape[1]
    lines = own.shape[1]
    low = jax.ShapeDtypeStruct((width + 8 * lines, LANES), jnp.bfloat16)
    return simple_call(
        join_body,
        (keep, got_a, got_b, own, *arrived),
        [
            jax.ShapeDtypeStruct((width, LANES), jnp.float32),
            jax.ShapeDtypeStruct((lines, 8, LANES), jnp.float32),
            low,
            low,
            low,
        ],
    )


def close_body(head, small, square, one, two, three, out, embed, shares, scalars):
    f32 = jnp.float32
    width = head.shape[0]
    lines = small.shape[0]
    across = width // LANES
    total = head[...]
    for side in (one, two, three):
        total = total + side[:width].astype(f32)
    out[...] = total.T
    rows = lines - shares.shape[1]
    part = jnp.zeros((8, LANES), f32)
    for t in range(lines):
        at = slice(width + 8 * t, width + 8 * t + 8)
        tile = small[t] + one[at].astype(f32) + two[at].astype(f32) + three[at].astype(f32)
        if t < rows:
            r, c = divmod(t, across)
            embed[8 * r : 8 * r + 8, c * LANES : (c + 1) * LANES] = tile
        else:
            low = tile.astype(shares.dtype)
            part = part + low.astype(f32) * low.astype(f32)
            for p in range(shares.shape[0]):
                shares[p, t - rows] = low
    column = lax.broadcasted_iota(jnp.int32, scalars.shape, 2)
    values = jnp.where(column == 1, square[0:1, :][None], jnp.sum(part))
    scalars[...] = jnp.where(column == 0, jnp.sum(total * total), values)


def close(head, small, square, arrived, peers, share):
    width = head.shape[0]
    rows = 8 * (small.shape[0] - share) * LANES // width
    return simple_call(
        close_body,
        (head, small, square, *arrived),
        [
            jax.ShapeDtypeStruct((LANES, width), jnp.float32),
            jax.ShapeDtypeStruct((rows, width), jnp.float32),
            jax.ShapeDtypeStruct((peers, share, 8, LANES), jnp.bfloat16),
            jax.ShapeDtypeStruct((peers, 1, LANES), jnp.float32),
        ],
    )


def subtotal_body(arrived, out):
    out[...] = jnp.sum(arrived[...], axis=0)


def subtotal(arrived):
    return simple_call(subtotal_body, (arrived,), [jax.ShapeDtypeStruct(arrived.shape[1:], jnp.float32)])[0]


def scale_body(counts, mine, two, one, three, head, embed, shares, head_grad, bias_grad, embed_grad, span_grad):
    f32 = jnp.float32
    totals = (mine[...] + two[...]) + (one[...] + three[...])

    def factor(k):
        mean = totals[:, k : k + 1] / counts[k] + EPSILON
        return jnp.minimum(1.0, 1.0 / jnp.sqrt(mean))

    head_grad[...] = factor(0) * head[...]
    embed_grad[...] = factor(1) * embed[...]
    rest = factor(2)
    across = span_grad.shape[1] // LANES
    share = shares.shape[1]
    for t in range(SPANS // 8 * across):
        r, c = divmod(t, across)
        tile = shares[t // share, t % share].astype(f32)
        span_grad[8 * r : 8 * r + 8, c * LANES : (c + 1) * LANES] = rest * tile
    t = SPANS // 8 * across
    bias_grad[...] = rest * shares[t // share, t % share].astype(f32)


def scale(counts, squares, head, embed, shares):
    width = head.shape[1]
    return simple_call(
        lambda *refs: scale_body(counts, *refs),
        (*squares, head, embed, shares),
        [
            jax.ShapeDtypeStruct(head.shape, jnp.float32),
            jax.ShapeDtypeStruct((width // LANES, LANES), jnp.float32),
            jax.ShapeDtypeStruct(embed.shape, jnp.float32),
            jax.ShapeDtypeStruct((SPANS, width), jnp.float32),
        ],
    )


def flipped(first, second):
    pairs = []
    for z in range(4):
        for x in range(4):
            pairs.append(((z * 4 + x) * 2, ((z ^ first[0]) * 4 + (x ^ first[1])) * 2))
            pairs.append(((z * 4 + x) * 2 + 1, ((z ^ second[0]) * 4 + (x ^ second[1])) * 2 + 1))
    return pairs


def along_u(x, k):
    return lax.ppermute(x, CLIENT, flipped((0, k), (k, 0)))


def along_v(x, k):
    return lax.ppermute(x, CLIENT, flipped((k, 0), (0, k)))


def to_core(x):
    return lax.ppermute(x, "client_2", [(0, 1), (1, 0)])


def along_head(x, low, high):
    axes = ("client_2", "head")
    pairs = [(h, h ^ low) for h in range(4)] + [(4 + h, 4 + (h ^ high)) for h in range(4)]
    return lax.ppermute(x, axes, pairs)


def wide(x):
    return x.astype(jnp.float32)


def narrow(x):
    return x.astype(jnp.bfloat16)


def to_head(x, k):
    return lax.ppermute(x, "head", [(h, h ^ k) for h in range(4)])


def exchange(x, axes):
    return lax.all_to_all(x, axes, 0, 0, tiled=True)


def per_device(pre, delta, head_weight, client_ids):
    hidden_width = pre.shape[1]
    emit_here = delta.shape[1]
    clients_here = client_ids.shape[0]
    head_devices = lax.axis_size("head")
    peers = lax.axis_size(CLIENT)
    share = -(-(SPANS // 8 * (emit_here // LANES) + 1) // peers)

    low, turned, bias_part = prepare(delta)
    part = partner_call(FIRST, pre, turned)
    arrived_first = to_core(part)
    part = partner_call(KEPT, pre, turned)
    arrived_kept = to_core(part)
    near, far = first_call(pre, turned, arrived_first)
    near = along_u(near, 1)
    far = along_u(far, 3)
    sent = slope_call(False, pre, low, head_weight)
    got = along_head(sent, 1, 3)
    kept = slope_call(True, pre, low, head_weight)
    message = narrow(kept[0] + wide(got[0]))
    got_two = along_head(message, 3, 1)
    send_a, send_b, keep = kept_call(pre, turned, arrived_kept, near, far)
    got_a = along_u(send_a, 3)
    got_b = along_u(send_b, 1)
    small_send, small_keep, embed_square = small_sends(
        kept, got, got_two, client_ids[None, :], bias_part, share
    )
    small_got = to_core(small_send)
    own, one, two, three = core_sum(small_keep, small_got)
    arrived = along_u(two, 2), along_u(one, 1), along_u(three, 3)
    final, small, one, two, three = join(keep, got_a, got_b, own, arrived)
    arrived = along_v(two, 2), along_v(one, 1), along_v(three, 3)
    head_raw, embed_raw, shares, scalars = close(final, small, embed_square, arrived, peers, share)
    scalars = exchange(scalars, CLIENT)
    shares = exchange(shares, CLIENT)
    squares = subtotal(scalars)
    squares = (squares, *(to_head(squares, k) for k in (2, 1, 3)))
    emit_total = emit_here * head_devices
    counts = (
        float(hidden_width * emit_total),
        float(clients_here * peers * hidden_width),
        float(SPANS * hidden_width + emit_total),
    )
    head_grad, bias_grad, embed_grad, span_grad = scale(counts, squares, head_raw, embed_raw, shares)
    return head_grad, bias_grad.reshape(emit_here), embed_grad, span_grad


def solution(mesh):
    torus = Mesh(
        mesh.devices.reshape(4, 4, 2, mesh.shape["head"]),
        ("client_0", "client_1", "client_2", "head"),
    )
    return jax.shard_map(
        per_device,
        mesh=torus,
        in_specs=(P(CLIENT, None), P(CLIENT, "head"), P(None, "head"), P(CLIENT)),
        out_specs=(P(CLIENT, "head"), P("head"), P(CLIENT, "head"), P(None, "head")),
        check_vma=False,
    )
```

```python
import jax
import jax.numpy as jnp
from jax import lax
from jax.experimental import pallas as pl
from jax.experimental.pallas import tpu as pltpu
from jax.sharding import Mesh
from jax.sharding import PartitionSpec as P

CLIENT = ("client_0", "client_1", "client_2")
EPSILON = 1e-06
LIMIT = 16 * 2**20
PREPARE_LIMIT = 44 * 2**20
LANES = 128

FIRST = ((2, 0), (2, 1), (1, 0), (1, 1), (2, 2), (2, 3), (3, 2), (3, 3))
ALL = tuple((u, v) for v in range(4) for u in range(4))
KEPT = ((3, 0), (3, 1), (0, 0), (0, 1), (1, 2), (1, 3), (0, 2), (0, 3))


def sigmoid(v):
    return 0.5 * jnp.tanh(0.5 * v) + 0.5


def params(limit=LIMIT):
    return pltpu.CompilerParams(dimension_semantics=("arbitrary",), vmem_limit_bytes=limit)


def whole():
    return pl.BlockSpec(memory_space=pltpu.VMEM)


PARTS = 5
STEP = 4
TILE = 1024
CHUNK = 320
SPANS = 80


def position():
    return tuple(lax.axis_index(a) for a in (*CLIENT, "head"))


def owner_at(side, u, v):
    z, x, _, _ = position()
    at_z = jnp.where(side == 0, z ^ v, z ^ u)
    at_x = jnp.where(side == 0, x ^ u, x ^ v)
    return (at_z * 4 + at_x) * 2 + side


def product(owners, pre, turned):
    units = []
    for owner in owners:
        v = pre[:, pl.ds(pl.multiple_of(owner * LANES, LANES), LANES)].astype(jnp.float32)
        units.append((v * sigmoid(v)).astype(jnp.bfloat16))
    return jnp.dot(turned[...], jnp.concatenate(units, axis=1), preferred_element_type=jnp.float32)


def pieces(acc):
    return [acc[:, j * LANES : (j + 1) * LANES] for j in range(acc.shape[1] // LANES)]


def prepare_body(delta, low, turned, sums, buffer, arrived):
    rows = delta.shape[0] // PARTS
    copies = [
        pltpu.make_async_copy(delta.at[pl.ds(k * rows, rows)], buffer.at[k], arrived.at[k]) for k in range(PARTS)
    ]
    for copy in copies:
        copy.start()
    total = None
    for k in range(PARTS):
        copies[k].wait()
        value = buffer[k]
        narrow = value.astype(jnp.bfloat16)
        low[k * rows : (k + 1) * rows, :] = narrow
        turned[:, k * rows : (k + 1) * rows] = narrow.T
        part = jnp.sum(value.reshape(rows // 8, 8, value.shape[1]), axis=0)
        total = part if total is None else total + part
    sums[...] = total


def prepare(delta):
    rows, width = delta.shape
    return pl.pallas_call(
        prepare_body,
        in_specs=[pl.BlockSpec(memory_space=pltpu.HBM)],
        out_specs=[whole()] * 3,
        out_shape=[
            jax.ShapeDtypeStruct((rows, width), jnp.bfloat16),
            jax.ShapeDtypeStruct((width, rows), jnp.bfloat16),
            jax.ShapeDtypeStruct((8, width), jnp.float32),
        ],
        scratch_shapes=[
            pltpu.VMEM((PARTS, rows // PARTS, width), jnp.float32),
            pltpu.SemaphoreType.DMA((PARTS,)),
        ],
        compiler_params=pltpu.CompilerParams(vmem_limit_bytes=PREPARE_LIMIT),
        cost_estimate=pl.CostEstimate(flops=8 * 10**9, bytes_accessed=2 * 10**7, transcendentals=0),
        name="prepare",
    )(delta)


def simple_call(body, operands, shapes):
    return pl.pallas_call(
        body,
        in_specs=[whole()] * len(operands),
        out_specs=[whole()] * len(shapes),
        out_shape=shapes,
        compiler_params=pltpu.CompilerParams(vmem_limit_bytes=LIMIT),
    )(*operands)


def partner_body(places, pre, turned, out):
    other = 1 - lax.axis_index("client_2")
    acc = product([owner_at(other, *place) for place in places], pre, turned)
    for j, piece in enumerate(pieces(acc)):
        out[j] = piece.astype(out.dtype)


def partner_call(places, pre, turned):
    shape = jax.ShapeDtypeStruct((len(places), turned.shape[0], LANES), jnp.bfloat16)
    return simple_call(lambda *refs: partner_body(places, *refs), (pre, turned), [shape])[0]


def first_body(pre, turned, arrived, near, far):
    core = lax.axis_index("client_2")
    acc = product([owner_at(core, *place) for place in FIRST], pre, turned)
    for j, piece in enumerate(pieces(acc)):
        out = near if j < STEP else far
        out[j % STEP] = (piece + arrived[j].astype(jnp.float32)).astype(out.dtype)


def first_call(pre, turned, arrived):
    shape = jax.ShapeDtypeStruct((STEP, turned.shape[0], LANES), jnp.bfloat16)
    return simple_call(first_body, (pre, turned, arrived), [shape, shape])


def kept_body(pre, turned, arrived, near, far, send_a, send_b, keep):
    core = lax.axis_index("client_2")
    acc = product([owner_at(core, *place) for place in KEPT], pre, turned)
    half = STEP // 2
    for j, piece in enumerate(pieces(acc)):
        side, send = (near, send_a) if j < STEP else (far, send_b)
        k = j % STEP
        total = piece + arrived[j].astype(jnp.float32) + side[k].astype(jnp.float32)
        if k < half:
            send[k] = total.astype(send.dtype)
        else:
            keep[j // STEP * half + k - half] = total.astype(keep.dtype)


def kept_call(pre, turned, arrived, near, far):
    width = turned.shape[0]
    half = jax.ShapeDtypeStruct((STEP // 2, width, LANES), jnp.bfloat16)
    full = jax.ShapeDtypeStruct((STEP, width, LANES), jnp.float32)
    return simple_call(kept_body, (pre, turned, arrived, near, far), [half, half, full])


def slope_body(kept, pre, low, weight, out):
    i = pl.program_id(0)
    _, _, core, head = position()
    rows, width = low.shape
    per = width // TILE
    clients = rows // SPANS
    if kept:
        first, second = jnp.where(core == 0, head ^ 3, head ^ 1), head
    else:
        first, second = head ^ 2, jnp.where(core == 0, head ^ 1, head ^ 3)
    at = pl.multiple_of((jnp.where(i < per, first, second) * per + i % per) * TILE, TILE)
    turned = weight[pl.ds(at, TILE), :].T
    put = pl.ds(pl.multiple_of((i % per) * TILE, TILE), TILE)
    spans = None
    for row in range(0, rows, CHUNK):
        part = jnp.dot(low[row : row + CHUNK, :], turned, preferred_element_type=jnp.float32)
        half = 0.5 * pre[row : row + CHUNK, pl.ds(at, TILE)].astype(jnp.float32)
        t = jnp.tanh(half)
        grad = part * ((1.0 + t) * (1.0 + half * (1.0 - t)))
        grad = grad.reshape(CHUNK // SPANS, SPANS, TILE)
        top = row // SPANS
        out[i // per, top : top + CHUNK // SPANS, put] = (0.5 * jnp.sum(grad, axis=1)).astype(out.dtype)
        some = jnp.sum(grad, axis=0)
        spans = some if spans is None else spans + some
    out[i // per, clients:, put] = (0.5 * spans).astype(out.dtype)


def slope_call(kept, pre, low, weight):
    rows, width = low.shape
    return pl.pallas_call(
        lambda *refs: slope_body(kept, *refs),
        grid=(2 * width // TILE,),
        in_specs=[whole()] * 3,
        out_specs=whole(),
        out_shape=jax.ShapeDtypeStruct((2, rows // SPANS + SPANS, width), jnp.float32 if kept else jnp.bfloat16),
        compiler_params=params(),
        name="slope_kept" if kept else "slope_sent",
    )(pre, low, weight)


def small_body(kept, got, got_two, ids, bias, send, keep, square, lines):
    f32 = jnp.float32
    core = lax.axis_index("client_2")
    sums = kept[1] + got[1].astype(f32) + got_two[...].astype(f32)
    width = sums.shape[1]
    across = width // LANES
    clients = ids.shape[1]
    count = 2 * send.shape[0]
    mine = sums[:clients]
    square[...] = jnp.full(square.shape, jnp.sum(mine * mine))
    line = lax.broadcasted_iota(jnp.int32, (count * clients, clients), 0)
    which = line // clients
    side = jnp.where(which < len(ALL), 1 - core, core)
    target = owner_at(side, which & 3, (which >> 2) & 3) * clients + line % clients
    selector = jnp.where(target == ids[...], 1.0, 0.0).astype(jnp.bfloat16)
    placed = jnp.dot(selector, mine.astype(jnp.bfloat16), preferred_element_type=f32)
    spans = sums[clients:]
    lines[...] = jnp.zeros(lines.shape, f32)
    for r in range(SPANS // 8):
        for c in range(across):
            lines[r * across + c] = spans[8 * r : 8 * r + 8, c * LANES : (c + 1) * LANES]
    bias_row = jnp.sum(bias[...], axis=0, keepdims=True)
    for c in range(across):
        lines[SPANS // 8 * across, c : c + 1, :] = bias_row[:, c * LANES : (c + 1) * LANES]
    groups = clients // 8
    share = send.shape[1] - groups * across
    for k in range(count):
        out = send if k < len(ALL) else keep
        at = k % len(ALL)
        for g in range(groups):
            for c in range(across):
                top = k * clients + 8 * g
                block = placed[top : top + 8, c * LANES : (c + 1) * LANES]
                out[at, g * across + c] = block.astype(out.dtype)
        owner = owner_at(1 - core if k < len(ALL) else core, *ALL[at])
        out[at, groups * across :] = lines[pl.ds(share * owner, share)].astype(out.dtype)


def small_sends(kept, got, got_two, ids, bias, share):
    width = kept.shape[2]
    tiles = ids.shape[1] // 8 * (width // LANES) + share
    shape = (len(ALL), tiles, 8, LANES)
    return pl.pallas_call(
        small_body,
        in_specs=[whole()] * 5,
        out_specs=[whole()] * 3,
        out_shape=[
            jax.ShapeDtypeStruct(shape, jnp.bfloat16),
            jax.ShapeDtypeStruct(shape, jnp.float32),
            jax.ShapeDtypeStruct((8, LANES), jnp.float32),
        ],
        scratch_shapes=[pltpu.VMEM((2 * len(ALL) * share, 8, LANES), jnp.float32)],
        compiler_params=pltpu.CompilerParams(vmem_limit_bytes=LIMIT),
        name="small_sends",
    )(kept, got, got_two, ids, bias)


def core_sum_body(keep, arrived, own, one, two, three):
    total = keep[...] + arrived[...].astype(jnp.float32)
    own[...] = total[0:4]
    for k, out in ((1, one), (2, two), (3, three)):
        out[...] = total[4 * k : 4 * k + 4].astype(out.dtype)


def core_sum(keep, arrived):
    shape = (keep.shape[0] // 4, *keep.shape[1:])
    low = jax.ShapeDtypeStruct(shape, jnp.bfloat16)
    return simple_call(core_sum_body, (keep, arrived), [jax.ShapeDtypeStruct(shape, jnp.float32), low, low, low])


def line_sum_body(own, side_one, side_two, side_three, mine, one, two, three):
    f32 = jnp.float32
    total = own[...] + side_one[...].astype(f32) + side_two[...].astype(f32) + side_three[...].astype(f32)
    mine[...] = total[0]
    for k, out in ((1, one), (2, two), (3, three)):
        out[...] = total[k].astype(out.dtype)


def line_sum(own, arrived):
    shape = own.shape[1:]
    low = jax.ShapeDtypeStruct(shape, jnp.bfloat16)
    return simple_call(line_sum_body, (own, *arrived), [jax.ShapeDtypeStruct(shape, jnp.float32), low, low, low])


def join_body(keep, got_a, got_b, head, one, two, three):
    for k, out in enumerate((head, one, two, three)):
        side = got_a if k < 2 else got_b
        out[...] = (keep[k] + side[k % 2].astype(jnp.float32)).astype(out.dtype)


def join(keep, got_a, got_b):
    low = jax.ShapeDtypeStruct(keep.shape[1:], jnp.bfloat16)
    own = jax.ShapeDtypeStruct(keep.shape[1:], jnp.float32)
    return simple_call(join_body, (keep, got_a, got_b), [own, low, low, low])


def close_body(head, one, two, three, small, s_one, s_two, s_three, square, total, embed, message):
    f32 = jnp.float32
    width = head.shape[0]
    lines = small.shape[0]
    across = width // LANES
    peers, share = message.shape[0], message.shape[1] - 1
    rows = lines - share
    part = jnp.zeros((8, LANES), f32)
    for t in range(lines):
        tile = small[t] + s_one[t].astype(f32) + s_two[t].astype(f32) + s_three[t].astype(f32)
        if t < rows:
            r, c = divmod(t, across)
            embed[8 * r : 8 * r + 8, c * LANES : (c + 1) * LANES] = tile
        else:
            low = tile.astype(message.dtype)
            part = part + low.astype(f32) * low.astype(f32)
            for p in range(peers):
                message[p, t - rows] = low
    value = head[...]
    for side in (one, two, three):
        value = value + side[...].astype(f32)
    total[...] = value
    column = lax.broadcasted_iota(jnp.int32, (8, LANES), 1)
    line = lax.broadcasted_iota(jnp.int32, (8, LANES), 0)
    sums = jnp.where(column == 1, square[...], jnp.sum(part))
    sums = jnp.where(column == 0, jnp.sum(value * value), sums)
    coarse = sums.astype(message.dtype).astype(f32)
    scalars = jnp.where(line == 0, coarse, jnp.where(line == 1, sums - coarse, 0.0)).astype(message.dtype)
    for p in range(peers):
        message[p, share] = scalars


def close(head, arrived, small, small_arrived, square, peers, share):
    width = head.shape[0]
    rows = 8 * (small.shape[0] - share) * LANES // width
    return simple_call(
        close_body,
        (head, *arrived, small, *small_arrived, square),
        [
            jax.ShapeDtypeStruct((width, LANES), jnp.float32),
            jax.ShapeDtypeStruct((rows, width), jnp.float32),
            jax.ShapeDtypeStruct((peers, share + 1, 8, LANES), jnp.bfloat16),
        ],
    )


def turn_body(value, out):
    out[...] = value[...].T


def turn(value):
    return simple_call(turn_body, (value,), [jax.ShapeDtypeStruct(value.shape[::-1], value.dtype)])[0]


def subtotal_body(arrived, out):
    last = arrived.shape[1] - 1
    total = None
    for p in range(arrived.shape[0]):
        some = arrived[p, last].astype(jnp.float32)
        total = some if total is None else total + some
    out[...] = jnp.sum(total, axis=0, keepdims=True)


def subtotal(arrived):
    shape = jax.ShapeDtypeStruct((1, arrived.shape[3]), jnp.float32)
    return simple_call(subtotal_body, (arrived,), [shape])[0]


def scale_body(counts, mine, two, one, three, head, embed, shares, head_grad, bias_grad, embed_grad, span_grad):
    f32 = jnp.float32
    totals = (mine[...] + two[...]) + (one[...] + three[...])

    def factor(k):
        mean = totals[:, k : k + 1] / counts[k] + EPSILON
        return jnp.minimum(1.0, 1.0 / jnp.sqrt(mean))

    head_grad[...] = factor(0) * head[...]
    embed_grad[...] = factor(1) * embed[...]
    rest = factor(2)
    across = span_grad.shape[1] // LANES
    share = shares.shape[1] - 1
    for t in range(SPANS // 8 * across):
        r, c = divmod(t, across)
        tile = shares[t // share, t % share].astype(f32)
        span_grad[8 * r : 8 * r + 8, c * LANES : (c + 1) * LANES] = rest * tile
    t = SPANS // 8 * across
    bias_grad[...] = rest * shares[t // share, t % share].astype(f32)


def scale(counts, squares, head, embed, shares):
    width = head.shape[1]
    return simple_call(
        lambda *refs: scale_body(counts, *refs),
        (*squares, head, embed, shares),
        [
            jax.ShapeDtypeStruct(head.shape, jnp.float32),
            jax.ShapeDtypeStruct((width // LANES, LANES), jnp.float32),
            jax.ShapeDtypeStruct(embed.shape, jnp.float32),
            jax.ShapeDtypeStruct((SPANS, width), jnp.float32),
        ],
    )


def flipped(first, second):
    pairs = []
    for z in range(4):
        for x in range(4):
            pairs.append(((z * 4 + x) * 2, ((z ^ first[0]) * 4 + (x ^ first[1])) * 2))
            pairs.append(((z * 4 + x) * 2 + 1, ((z ^ second[0]) * 4 + (x ^ second[1])) * 2 + 1))
    return pairs


def along_u(x, k):
    return lax.ppermute(x, CLIENT, flipped((0, k), (k, 0)))


def along_v(x, k):
    return lax.ppermute(x, CLIENT, flipped((k, 0), (0, k)))


def to_core(x):
    return lax.ppermute(x, "client_2", [(0, 1), (1, 0)])


def along_head(x, low, high):
    axes = ("client_2", "head")
    pairs = [(h, h ^ low) for h in range(4)] + [(4 + h, 4 + (h ^ high)) for h in range(4)]
    return lax.ppermute(x, axes, pairs)


def wide(x):
    return x.astype(jnp.float32)


def narrow(x):
    return x.astype(jnp.bfloat16)


def to_head(x, k):
    return lax.ppermute(x, "head", [(h, h ^ k) for h in range(4)])


def exchange(x, axes):
    return lax.all_to_all(x, axes, 0, 0, tiled=True)


def per_device(pre, delta, head_weight, client_ids):
    hidden_width = pre.shape[1]
    emit_here = delta.shape[1]
    clients_here = client_ids.shape[0]
    head_devices = lax.axis_size("head")
    peers = lax.axis_size(CLIENT)
    share = -(-(SPANS // 8 * (emit_here // LANES) + 1) // peers)

    low, turned, bias_part = prepare(delta)
    part = partner_call(FIRST, pre, turned)
    arrived_first = to_core(part)
    part = partner_call(KEPT, pre, turned)
    arrived_kept = to_core(part)
    near, far = first_call(pre, turned, arrived_first)
    near = along_u(near, 1)
    far = along_u(far, 3)
    sent = slope_call(False, pre, low, head_weight)
    got = along_head(sent, 1, 3)
    kept = slope_call(True, pre, low, head_weight)
    message = narrow(kept[0] + wide(got[0]))
    got_two = along_head(message, 3, 1)
    send_a, send_b, keep = kept_call(pre, turned, arrived_kept, near, far)
    got_a = along_u(send_a, 3)
    got_b = along_u(send_b, 1)
    small_send, small_keep, embed_square = small_sends(kept, got, got_two, client_ids[None, :], bias_part, share)
    small_got = to_core(small_send)
    own, one, two, three = core_sum(small_keep, small_got)
    small_arrived = along_v(one, 1), along_v(two, 2), along_v(three, 3)
    final, one, two, three = join(keep, got_a, got_b)
    arrived = along_v(one, 1), along_v(two, 2), along_v(three, 3)
    small, one, two, three = line_sum(own, small_arrived)
    small_arrived = along_u(one, 1), along_u(two, 2), along_u(three, 3)
    total, embed_raw, message = close(final, arrived, small, small_arrived, embed_square, peers, share)
    shares = exchange(message, CLIENT)
    head_raw = turn(total)
    squares = subtotal(shares)
    squares = (squares, *(to_head(squares, k) for k in (2, 1, 3)))
    emit_total = emit_here * head_devices
    counts = (
        float(hidden_width * emit_total),
        float(clients_here * peers * hidden_width),
        float(SPANS * hidden_width + emit_total),
    )
    head_grad, bias_grad, embed_grad, span_grad = scale(counts, squares, head_raw, embed_raw, shares)
    return head_grad, bias_grad.reshape(emit_here), embed_grad, span_grad


def solution(mesh):
    torus = Mesh(
        mesh.devices.reshape(4, 4, 2, mesh.shape["head"]),
        ("client_0", "client_1", "client_2", "head"),
    )
    return jax.shard_map(
        per_device,
        mesh=torus,
        in_specs=(P(CLIENT, None), P(CLIENT, "head"), P(None, "head"), P(CLIENT)),
        out_specs=(P(CLIENT, "head"), P("head"), P(CLIENT, "head"), P(None, "head")),
        check_vma=False,
    )
```

```python
import jax
import jax.numpy as jnp
from jax import lax
from jax.experimental import pallas as pl
from jax.experimental.pallas import tpu as pltpu
from jax.sharding import Mesh
from jax.sharding import PartitionSpec as P

CLIENT = ("client_0", "client_1", "client_2")
EPSILON = 1e-06
LIMIT = 16 * 2**20
PREPARE_LIMIT = 46 * 2**20
LANES = 128

FIRST = ((2, 0), (2, 1), (1, 0), (1, 1), (2, 2), (2, 3), (3, 2), (3, 3))
ALL = tuple((u, v) for v in range(4) for u in range(4))
KEPT = ((3, 0), (3, 1), (0, 0), (0, 1), (1, 2), (1, 3), (0, 2), (0, 3))


def sigmoid(v):
    return 0.5 * jnp.tanh(0.5 * v) + 0.5


def params(limit=LIMIT):
    return pltpu.CompilerParams(dimension_semantics=("arbitrary",), vmem_limit_bytes=limit)


def whole():
    return pl.BlockSpec(memory_space=pltpu.VMEM)


PARTS = 5
STEP = 4
TILE = 1024
CHUNK = 320
SPANS = 80


def position():
    return tuple(lax.axis_index(a) for a in (*CLIENT, "head"))


def owner_at(side, u, v):
    z, x, _, _ = position()
    at_z = jnp.where(side == 0, z ^ v, z ^ u)
    at_x = jnp.where(side == 0, x ^ u, x ^ v)
    return (at_z * 4 + at_x) * 2 + side


def product(owners, pre, turned):
    units = []
    for owner in owners:
        at = owner * LANES if isinstance(owner, int) else pl.multiple_of(owner * LANES, LANES)
        v = pre[:, pl.ds(at, LANES)].astype(jnp.float32)
        units.append((v * sigmoid(v)).astype(jnp.bfloat16))
    return jnp.dot(turned[...], jnp.concatenate(units, axis=1), preferred_element_type=jnp.float32)


def pieces(acc):
    return [acc[:, j * LANES : (j + 1) * LANES] for j in range(acc.shape[1] // LANES)]


def prepare_body(delta, source, low, turned, sums, early, buffer, arrived, loaded):
    rows = delta.shape[0] // PARTS
    copies = [
        pltpu.make_async_copy(delta.at[pl.ds(k * rows, rows)], buffer.at[k], arrived.at[k]) for k in range(PARTS)
    ]
    for copy in copies:
        copy.start()
    other = 1 - lax.axis_index("client_2")
    loads = []
    for k, place in enumerate(FIRST):
        at = pl.ds(pl.multiple_of(owner_at(other, *place) * LANES, LANES), LANES)
        to = slice(k * LANES, (k + 1) * LANES)
        loads.append(pltpu.make_async_copy(source.at[:, at], early.at[:, to], loaded.at[k]))
        loads[-1].start()
    total = None
    for k in range(PARTS):
        copies[k].wait()
        value = buffer[k]
        narrow = value.astype(jnp.bfloat16)
        low[k * rows : (k + 1) * rows, :] = narrow
        turned[:, k * rows : (k + 1) * rows] = narrow.T
        part = jnp.sum(value.reshape(rows // 8, 8, value.shape[1]), axis=0)
        total = part if total is None else total + part
    sums[...] = total
    for load in loads:
        load.wait()


def prepare(delta, pre):
    rows, width = delta.shape
    return pl.pallas_call(
        prepare_body,
        in_specs=[pl.BlockSpec(memory_space=pltpu.HBM)] * 2,
        out_specs=[whole()] * 4,
        out_shape=[
            jax.ShapeDtypeStruct((rows, width), jnp.bfloat16),
            jax.ShapeDtypeStruct((width, rows), jnp.bfloat16),
            jax.ShapeDtypeStruct((8, width), jnp.float32),
            jax.ShapeDtypeStruct((rows, len(FIRST) * LANES), pre.dtype),
        ],
        scratch_shapes=[
            pltpu.VMEM((PARTS, rows // PARTS, width), jnp.float32),
            pltpu.SemaphoreType.DMA((PARTS,)),
            pltpu.SemaphoreType.DMA((len(FIRST),)),
        ],
        compiler_params=pltpu.CompilerParams(vmem_limit_bytes=PREPARE_LIMIT),
        cost_estimate=pl.CostEstimate(flops=8 * 10**9, bytes_accessed=2 * 10**7, transcendentals=0),
        name="prepare",
    )(delta, pre)


def simple_call(body, operands, shapes):
    return pl.pallas_call(
        body,
        in_specs=[whole()] * len(operands),
        out_specs=[whole()] * len(shapes),
        out_shape=shapes,
        compiler_params=pltpu.CompilerParams(vmem_limit_bytes=LIMIT),
    )(*operands)


def partner_body(owners, pre, turned, out):
    acc = product(owners(), pre, turned)
    for j, piece in enumerate(pieces(acc)):
        out[j] = piece.astype(out.dtype)


def partner_call(owners, pre, turned):
    shape = jax.ShapeDtypeStruct((len(FIRST), turned.shape[0], LANES), jnp.bfloat16)
    return simple_call(lambda *refs: partner_body(owners, *refs), (pre, turned), [shape])[0]


def partner_kept():
    return [owner_at(1 - lax.axis_index("client_2"), *place) for place in KEPT]


def first_body(pre, turned, arrived, near, far):
    core = lax.axis_index("client_2")
    acc = product([owner_at(core, *place) for place in FIRST], pre, turned)
    for j, piece in enumerate(pieces(acc)):
        out = near if j < STEP else far
        out[j % STEP] = (piece + arrived[j].astype(jnp.float32)).astype(out.dtype)


def first_call(pre, turned, arrived):
    shape = jax.ShapeDtypeStruct((STEP, turned.shape[0], LANES), jnp.bfloat16)
    return simple_call(first_body, (pre, turned, arrived), [shape, shape])


def kept_body(pre, turned, arrived, near, far, send_a, send_b, keep):
    core = lax.axis_index("client_2")
    acc = product([owner_at(core, *place) for place in KEPT], pre, turned)
    half = STEP // 2
    for j, piece in enumerate(pieces(acc)):
        side, send = (near, send_a) if j < STEP else (far, send_b)
        k = j % STEP
        total = piece + arrived[j].astype(jnp.float32) + side[k].astype(jnp.float32)
        if k < half:
            send[k] = total.astype(send.dtype)
        else:
            keep[j // STEP * half + k - half] = total.astype(keep.dtype)


def kept_call(pre, turned, arrived, near, far):
    width = turned.shape[0]
    half = jax.ShapeDtypeStruct((STEP // 2, width, LANES), jnp.bfloat16)
    full = jax.ShapeDtypeStruct((STEP, width, LANES), jnp.float32)
    return simple_call(kept_body, (pre, turned, arrived, near, far), [half, half, full])


def slope_body(kept, pre, low, weight, out):
    i = pl.program_id(0)
    _, _, core, head = position()
    rows, width = low.shape
    per = width // TILE
    clients = rows // SPANS
    if kept:
        first, second = jnp.where(core == 0, head ^ 3, head ^ 1), head
    else:
        first, second = head ^ 2, jnp.where(core == 0, head ^ 1, head ^ 3)
    at = pl.multiple_of((jnp.where(i < per, first, second) * per + i % per) * TILE, TILE)
    turned = weight[pl.ds(at, TILE), :].T
    put = pl.ds(pl.multiple_of((i % per) * TILE, TILE), TILE)
    spans = None
    for row in range(0, rows, CHUNK):
        part = jnp.dot(low[row : row + CHUNK, :], turned, preferred_element_type=jnp.float32)
        half = 0.5 * pre[row : row + CHUNK, pl.ds(at, TILE)].astype(jnp.float32)
        t = jnp.tanh(half)
        grad = part * ((1.0 + t) * (1.0 + half * (1.0 - t)))
        grad = grad.reshape(CHUNK // SPANS, SPANS, TILE)
        top = row // SPANS
        out[i // per, top : top + CHUNK // SPANS, put] = (0.5 * jnp.sum(grad, axis=1)).astype(out.dtype)
        some = jnp.sum(grad, axis=0)
        spans = some if spans is None else spans + some
    out[i // per, clients:, put] = (0.5 * spans).astype(out.dtype)


def slope_call(kept, pre, low, weight):
    rows, width = low.shape
    return pl.pallas_call(
        lambda *refs: slope_body(kept, *refs),
        grid=(2 * width // TILE,),
        in_specs=[whole()] * 3,
        out_specs=whole(),
        out_shape=jax.ShapeDtypeStruct((2, rows // SPANS + SPANS, width), jnp.float32 if kept else jnp.bfloat16),
        compiler_params=params(),
        name="slope_kept" if kept else "slope_sent",
    )(pre, low, weight)


def small_body(kept, got, got_two, ids, bias, send, keep, square, lines):
    f32 = jnp.float32
    core = lax.axis_index("client_2")
    sums = kept[1] + got[1].astype(f32) + got_two[...].astype(f32)
    width = sums.shape[1]
    across = width // LANES
    clients = ids.shape[1]
    count = 2 * send.shape[0]
    mine = sums[:clients]
    square[...] = jnp.full(square.shape, jnp.sum(mine * mine))
    line = lax.broadcasted_iota(jnp.int32, (count * clients, clients), 0)
    which = line // clients
    side = jnp.where(which < len(ALL), 1 - core, core)
    target = owner_at(side, which & 3, (which >> 2) & 3) * clients + line % clients
    selector = jnp.where(target == ids[...], 1.0, 0.0).astype(jnp.bfloat16)
    placed = jnp.dot(selector, mine.astype(jnp.bfloat16), preferred_element_type=f32)
    spans = sums[clients:]
    lines[...] = jnp.zeros(lines.shape, f32)
    for r in range(SPANS // 8):
        for c in range(across):
            lines[r * across + c] = spans[8 * r : 8 * r + 8, c * LANES : (c + 1) * LANES]
    bias_row = jnp.sum(bias[...], axis=0, keepdims=True)
    for c in range(across):
        lines[SPANS // 8 * across, c : c + 1, :] = bias_row[:, c * LANES : (c + 1) * LANES]
    groups = clients // 8
    share = send.shape[1] - groups * across
    for k in range(count):
        out = send if k < len(ALL) else keep
        at = k % len(ALL)
        for g in range(groups):
            for c in range(across):
                top = k * clients + 8 * g
                block = placed[top : top + 8, c * LANES : (c + 1) * LANES]
                out[at, g * across + c] = block.astype(out.dtype)
        owner = owner_at(1 - core if k < len(ALL) else core, *ALL[at])
        out[at, groups * across :] = lines[pl.ds(share * owner, share)].astype(out.dtype)


def small_sends(kept, got, got_two, ids, bias, share):
    width = kept.shape[2]
    tiles = ids.shape[1] // 8 * (width // LANES) + share
    shape = (len(ALL), tiles, 8, LANES)
    return pl.pallas_call(
        small_body,
        in_specs=[whole()] * 5,
        out_specs=[whole()] * 3,
        out_shape=[
            jax.ShapeDtypeStruct(shape, jnp.bfloat16),
            jax.ShapeDtypeStruct(shape, jnp.float32),
            jax.ShapeDtypeStruct((8, LANES), jnp.float32),
        ],
        scratch_shapes=[pltpu.VMEM((2 * len(ALL) * share, 8, LANES), jnp.float32)],
        compiler_params=pltpu.CompilerParams(vmem_limit_bytes=LIMIT),
        name="small_sends",
    )(kept, got, got_two, ids, bias)


def core_sum_body(keep, arrived, own, one, two, three):
    total = keep[...] + arrived[...].astype(jnp.float32)
    own[...] = total[0:4]
    for k, out in ((1, one), (2, two), (3, three)):
        out[...] = total[4 * k : 4 * k + 4].astype(out.dtype)


def core_sum(keep, arrived):
    shape = (keep.shape[0] // 4, *keep.shape[1:])
    low = jax.ShapeDtypeStruct(shape, jnp.bfloat16)
    return simple_call(core_sum_body, (keep, arrived), [jax.ShapeDtypeStruct(shape, jnp.float32), low, low, low])


def line_sum_body(own, side_one, side_two, side_three, mine, one, two, three):
    f32 = jnp.float32
    total = own[...] + side_one[...].astype(f32) + side_two[...].astype(f32) + side_three[...].astype(f32)
    mine[...] = total[0]
    for k, out in ((1, one), (2, two), (3, three)):
        out[...] = total[k].astype(out.dtype)


def line_sum(own, arrived):
    shape = own.shape[1:]
    low = jax.ShapeDtypeStruct(shape, jnp.bfloat16)
    return simple_call(line_sum_body, (own, *arrived), [jax.ShapeDtypeStruct(shape, jnp.float32), low, low, low])


def join_body(keep, got_a, got_b, head, one, two, three):
    for k, out in enumerate((head, one, two, three)):
        side = got_a if k < 2 else got_b
        out[...] = (keep[k] + side[k % 2].astype(jnp.float32)).astype(out.dtype)


def join(keep, got_a, got_b):
    low = jax.ShapeDtypeStruct(keep.shape[1:], jnp.bfloat16)
    own = jax.ShapeDtypeStruct(keep.shape[1:], jnp.float32)
    return simple_call(join_body, (keep, got_a, got_b), [own, low, low, low])


def close_body(head, one, two, three, small, s_one, s_two, s_three, square, total, embed, message):
    f32 = jnp.float32
    width = head.shape[0]
    lines = small.shape[0]
    across = width // LANES
    peers, share = message.shape[0], message.shape[1] - 1
    rows = lines - share
    part = jnp.zeros((8, LANES), f32)
    for t in range(lines):
        tile = small[t] + s_one[t].astype(f32) + s_two[t].astype(f32) + s_three[t].astype(f32)
        if t < rows:
            r, c = divmod(t, across)
            embed[8 * r : 8 * r + 8, c * LANES : (c + 1) * LANES] = tile
        else:
            low = tile.astype(message.dtype)
            part = part + low.astype(f32) * low.astype(f32)
            for p in range(peers):
                message[p, t - rows] = low
    value = head[...]
    for side in (one, two, three):
        value = value + side[...].astype(f32)
    total[...] = value
    column = lax.broadcasted_iota(jnp.int32, (8, LANES), 1)
    line = lax.broadcasted_iota(jnp.int32, (8, LANES), 0)
    sums = jnp.where(column == 1, square[...], jnp.sum(part))
    sums = jnp.where(column == 0, jnp.sum(value * value), sums)
    coarse = sums.astype(message.dtype).astype(f32)
    scalars = jnp.where(line == 0, coarse, jnp.where(line == 1, sums - coarse, 0.0)).astype(message.dtype)
    for p in range(peers):
        message[p, share] = scalars


def close(head, arrived, small, small_arrived, square, peers, share):
    width = head.shape[0]
    rows = 8 * (small.shape[0] - share) * LANES // width
    return simple_call(
        close_body,
        (head, *arrived, small, *small_arrived, square),
        [
            jax.ShapeDtypeStruct((width, LANES), jnp.float32),
            jax.ShapeDtypeStruct((rows, width), jnp.float32),
            jax.ShapeDtypeStruct((peers, share + 1, 8, LANES), jnp.bfloat16),
        ],
    )


def turn_body(value, out):
    out[...] = value[...].T


def turn(value):
    return simple_call(turn_body, (value,), [jax.ShapeDtypeStruct(value.shape[::-1], value.dtype)])[0]


def subtotal_body(arrived, out):
    last = arrived.shape[1] - 1
    total = None
    for p in range(arrived.shape[0]):
        some = arrived[p, last].astype(jnp.float32)
        total = some if total is None else total + some
    out[...] = jnp.sum(total, axis=0, keepdims=True)


def subtotal(arrived):
    shape = jax.ShapeDtypeStruct((1, arrived.shape[3]), jnp.float32)
    return simple_call(subtotal_body, (arrived,), [shape])[0]


def scale_body(counts, mine, two, one, three, head, embed, shares, head_grad, bias_grad, embed_grad, span_grad):
    f32 = jnp.float32
    totals = (mine[...] + two[...]) + (one[...] + three[...])

    def factor(k):
        mean = totals[:, k : k + 1] / counts[k] + EPSILON
        return jnp.minimum(1.0, 1.0 / jnp.sqrt(mean))

    head_grad[...] = factor(0) * head[...]
    embed_grad[...] = factor(1) * embed[...]
    rest = factor(2)
    across = span_grad.shape[1] // LANES
    share = shares.shape[1] - 1
    for t in range(SPANS // 8 * across):
        r, c = divmod(t, across)
        tile = shares[t // share, t % share].astype(f32)
        span_grad[8 * r : 8 * r + 8, c * LANES : (c + 1) * LANES] = rest * tile
    t = SPANS // 8 * across
    bias_grad[...] = rest * shares[t // share, t % share].astype(f32)


def scale(counts, squares, head, embed, shares):
    width = head.shape[1]
    return simple_call(
        lambda *refs: scale_body(counts, *refs),
        (*squares, head, embed, shares),
        [
            jax.ShapeDtypeStruct(head.shape, jnp.float32),
            jax.ShapeDtypeStruct((width // LANES, LANES), jnp.float32),
            jax.ShapeDtypeStruct(embed.shape, jnp.float32),
            jax.ShapeDtypeStruct((SPANS, width), jnp.float32),
        ],
    )


def flipped(first, second):
    pairs = []
    for z in range(4):
        for x in range(4):
            pairs.append(((z * 4 + x) * 2, ((z ^ first[0]) * 4 + (x ^ first[1])) * 2))
            pairs.append(((z * 4 + x) * 2 + 1, ((z ^ second[0]) * 4 + (x ^ second[1])) * 2 + 1))
    return pairs


def along_u(x, k):
    return lax.ppermute(x, CLIENT, flipped((0, k), (k, 0)))


def along_v(x, k):
    return lax.ppermute(x, CLIENT, flipped((k, 0), (0, k)))


def to_core(x):
    return lax.ppermute(x, "client_2", [(0, 1), (1, 0)])


def along_head(x, low, high):
    axes = ("client_2", "head")
    pairs = [(h, h ^ low) for h in range(4)] + [(4 + h, 4 + (h ^ high)) for h in range(4)]
    return lax.ppermute(x, axes, pairs)


def wide(x):
    return x.astype(jnp.float32)


def narrow(x):
    return x.astype(jnp.bfloat16)


def to_head(x, k):
    return lax.ppermute(x, "head", [(h, h ^ k) for h in range(4)])


def exchange(x, axes):
    return lax.all_to_all(x, axes, 0, 0, tiled=True)


def per_device(pre, delta, head_weight, client_ids):
    hidden_width = pre.shape[1]
    emit_here = delta.shape[1]
    clients_here = client_ids.shape[0]
    head_devices = lax.axis_size("head")
    peers = lax.axis_size(CLIENT)
    share = -(-(SPANS // 8 * (emit_here // LANES) + 1) // peers)

    low, turned, bias_part, early = prepare(delta, pre)
    part = partner_call(lambda: range(len(FIRST)), early, turned)
    arrived_first = to_core(part)
    part = partner_call(partner_kept, pre, turned)
    arrived_kept = to_core(part)
    near, far = first_call(pre, turned, arrived_first)
    near = along_u(near, 1)
    far = along_u(far, 3)
    sent = slope_call(False, pre, low, head_weight)
    got = along_head(sent, 1, 3)
    kept = slope_call(True, pre, low, head_weight)
    message = narrow(kept[0] + wide(got[0]))
    got_two = along_head(message, 3, 1)
    send_a, send_b, keep = kept_call(pre, turned, arrived_kept, near, far)
    got_a = along_u(send_a, 3)
    got_b = along_u(send_b, 1)
    small_send, small_keep, embed_square = small_sends(kept, got, got_two, client_ids[None, :], bias_part, share)
    small_got = to_core(small_send)
    own, one, two, three = core_sum(small_keep, small_got)
    small_arrived = along_v(one, 1), along_v(two, 2), along_v(three, 3)
    final, one, two, three = join(keep, got_a, got_b)
    arrived = along_v(one, 1), along_v(two, 2), along_v(three, 3)
    small, one, two, three = line_sum(own, small_arrived)
    small_arrived = along_u(one, 1), along_u(two, 2), along_u(three, 3)
    total, embed_raw, message = close(final, arrived, small, small_arrived, embed_square, peers, share)
    shares = exchange(message, CLIENT)
    head_raw = turn(total)
    squares = subtotal(shares)
    squares = (squares, *(to_head(squares, k) for k in (2, 1, 3)))
    emit_total = emit_here * head_devices
    counts = (
        float(hidden_width * emit_total),
        float(clients_here * peers * hidden_width),
        float(SPANS * hidden_width + emit_total),
    )
    head_grad, bias_grad, embed_grad, span_grad = scale(counts, squares, head_raw, embed_raw, shares)
    return head_grad, bias_grad.reshape(emit_here), embed_grad, span_grad


def solution(mesh):
    torus = Mesh(
        mesh.devices.reshape(4, 4, 2, mesh.shape["head"]),
        ("client_0", "client_1", "client_2", "head"),
    )
    return jax.shard_map(
        per_device,
        mesh=torus,
        in_specs=(P(CLIENT, None), P(CLIENT, "head"), P(None, "head"), P(CLIENT)),
        out_specs=(P(CLIENT, "head"), P("head"), P(CLIENT, "head"), P(None, "head")),
        check_vma=False,
    )
```

```python
import jax
import jax.numpy as jnp
from jax import lax
from jax.experimental import pallas as pl
from jax.experimental.pallas import tpu as pltpu
from jax.sharding import Mesh
from jax.sharding import PartitionSpec as P

CLIENT = ("client_0", "client_1", "client_2")
EPSILON = 1e-06
LIMIT = 16 * 2**20
PREPARE_LIMIT = 46 * 2**20
LANES = 128

FIRST = ((2, 0), (2, 1), (1, 0), (1, 1), (2, 2), (2, 3), (3, 2), (3, 3))
ALL = tuple((u, v) for v in range(4) for u in range(4))
KEPT = ((3, 0), (3, 1), (0, 0), (0, 1), (1, 2), (1, 3), (0, 2), (0, 3))


def sigmoid(v):
    return 0.5 * jnp.tanh(0.5 * v) + 0.5


def params(limit=LIMIT):
    return pltpu.CompilerParams(dimension_semantics=("arbitrary",), vmem_limit_bytes=limit)


def whole():
    return pl.BlockSpec(memory_space=pltpu.VMEM)


PARTS = 10
STEP = 4
TILE = 1024
CHUNK = 320
SPANS = 80


def position():
    return tuple(lax.axis_index(a) for a in (*CLIENT, "head"))


def owner_at(side, u, v):
    z, x, _, _ = position()
    at_z = jnp.where(side == 0, z ^ v, z ^ u)
    at_x = jnp.where(side == 0, x ^ u, x ^ v)
    return (at_z * 4 + at_x) * 2 + side


def product(owners, pre, turned):
    units = []
    for owner in owners:
        at = owner * LANES if isinstance(owner, int) else pl.multiple_of(owner * LANES, LANES)
        v = pre[:, pl.ds(at, LANES)].astype(jnp.float32)
        units.append((v * sigmoid(v)).astype(jnp.bfloat16))
    return jnp.dot(turned[...], jnp.concatenate(units, axis=1), preferred_element_type=jnp.float32)


def pieces(acc):
    return [acc[:, j * LANES : (j + 1) * LANES] for j in range(acc.shape[1] // LANES)]


def prepare_body(delta, source, low, turned, sums, early, buffer, arrived, loaded):
    rows = delta.shape[0] // PARTS
    copies = [
        pltpu.make_async_copy(delta.at[pl.ds(k * rows, rows)], buffer.at[k], arrived.at[k]) for k in range(PARTS)
    ]
    for copy in copies:
        copy.start()
    other = 1 - lax.axis_index("client_2")
    loads = []
    for k, place in enumerate(FIRST):
        at = pl.ds(pl.multiple_of(owner_at(other, *place) * LANES, LANES), LANES)
        to = slice(k * LANES, (k + 1) * LANES)
        loads.append(pltpu.make_async_copy(source.at[:, at], early.at[:, to], loaded.at[k]))
        loads[-1].start()
    total = None
    for k in range(PARTS):
        copies[k].wait()
        value = buffer[k]
        narrow = value.astype(jnp.bfloat16)
        low[k * rows : (k + 1) * rows, :] = narrow
        turned[:, k * rows : (k + 1) * rows] = narrow.T
        part = jnp.sum(value.reshape(rows // 8, 8, value.shape[1]), axis=0)
        total = part if total is None else total + part
    sums[...] = total
    for load in loads:
        load.wait()


def prepare(delta, pre):
    rows, width = delta.shape
    return pl.pallas_call(
        prepare_body,
        in_specs=[pl.BlockSpec(memory_space=pltpu.HBM)] * 2,
        out_specs=[whole()] * 4,
        out_shape=[
            jax.ShapeDtypeStruct((rows, width), jnp.bfloat16),
            jax.ShapeDtypeStruct((width, rows), jnp.bfloat16),
            jax.ShapeDtypeStruct((8, width), jnp.float32),
            jax.ShapeDtypeStruct((rows, len(FIRST) * LANES), pre.dtype),
        ],
        scratch_shapes=[
            pltpu.VMEM((PARTS, rows // PARTS, width), jnp.float32),
            pltpu.SemaphoreType.DMA((PARTS,)),
            pltpu.SemaphoreType.DMA((len(FIRST),)),
        ],
        compiler_params=pltpu.CompilerParams(vmem_limit_bytes=PREPARE_LIMIT),
        cost_estimate=pl.CostEstimate(flops=8 * 10**9, bytes_accessed=2 * 10**7, transcendentals=0),
        name="prepare",
    )(delta, pre)


def simple_call(body, operands, shapes):
    return pl.pallas_call(
        body,
        in_specs=[whole()] * len(operands),
        out_specs=[whole()] * len(shapes),
        out_shape=shapes,
        compiler_params=pltpu.CompilerParams(vmem_limit_bytes=LIMIT),
    )(*operands)


def partner_body(owners, pre, turned, out):
    acc = product(owners(), pre, turned)
    for j, piece in enumerate(pieces(acc)):
        out[j] = piece.astype(out.dtype)


def partner_call(owners, pre, turned):
    shape = jax.ShapeDtypeStruct((len(FIRST), turned.shape[0], LANES), jnp.bfloat16)
    return simple_call(lambda *refs: partner_body(owners, *refs), (pre, turned), [shape])[0]


def partner_kept():
    return [owner_at(1 - lax.axis_index("client_2"), *place) for place in KEPT]


def first_body(pre, turned, arrived, near, far):
    core = lax.axis_index("client_2")
    acc = product([owner_at(core, *place) for place in FIRST], pre, turned)
    for j, piece in enumerate(pieces(acc)):
        out = near if j < STEP else far
        out[j % STEP] = (piece + arrived[j].astype(jnp.float32)).astype(out.dtype)


def first_call(pre, turned, arrived):
    shape = jax.ShapeDtypeStruct((STEP, turned.shape[0], LANES), jnp.bfloat16)
    return simple_call(first_body, (pre, turned, arrived), [shape, shape])


def kept_body(pre, turned, arrived, near, far, send_a, send_b, keep):
    core = lax.axis_index("client_2")
    acc = product([owner_at(core, *place) for place in KEPT], pre, turned)
    half = STEP // 2
    for j, piece in enumerate(pieces(acc)):
        side, send = (near, send_a) if j < STEP else (far, send_b)
        k = j % STEP
        total = piece + arrived[j].astype(jnp.float32) + side[k].astype(jnp.float32)
        if k < half:
            send[k] = total.astype(send.dtype)
        else:
            keep[j // STEP * half + k - half] = total.astype(keep.dtype)


def kept_call(pre, turned, arrived, near, far):
    width = turned.shape[0]
    half = jax.ShapeDtypeStruct((STEP // 2, width, LANES), jnp.bfloat16)
    full = jax.ShapeDtypeStruct((STEP, width, LANES), jnp.float32)
    return simple_call(kept_body, (pre, turned, arrived, near, far), [half, half, full])


def slope_body(kept, pre, low, weight, out):
    i = pl.program_id(0)
    _, _, core, head = position()
    rows, width = low.shape
    per = width // TILE
    clients = rows // SPANS
    if kept:
        first, second = jnp.where(core == 0, head ^ 3, head ^ 1), head
    else:
        first, second = head ^ 2, jnp.where(core == 0, head ^ 1, head ^ 3)
    at = pl.multiple_of((jnp.where(i < per, first, second) * per + i % per) * TILE, TILE)
    turned = weight[pl.ds(at, TILE), :].T
    put = pl.ds(pl.multiple_of((i % per) * TILE, TILE), TILE)
    spans = None
    for row in range(0, rows, CHUNK):
        part = jnp.dot(low[row : row + CHUNK, :], turned, preferred_element_type=jnp.float32)
        half = 0.5 * pre[row : row + CHUNK, pl.ds(at, TILE)].astype(jnp.float32)
        t = jnp.tanh(half)
        grad = part * ((1.0 + t) * (1.0 + half * (1.0 - t)))
        grad = grad.reshape(CHUNK // SPANS, SPANS, TILE)
        top = row // SPANS
        out[i // per, top : top + CHUNK // SPANS, put] = (0.5 * jnp.sum(grad, axis=1)).astype(out.dtype)
        some = jnp.sum(grad, axis=0)
        spans = some if spans is None else spans + some
    out[i // per, clients:, put] = (0.5 * spans).astype(out.dtype)


def slope_call(kept, pre, low, weight):
    rows, width = low.shape
    return pl.pallas_call(
        lambda *refs: slope_body(kept, *refs),
        grid=(2 * width // TILE,),
        in_specs=[whole()] * 3,
        out_specs=whole(),
        out_shape=jax.ShapeDtypeStruct((2, rows // SPANS + SPANS, width), jnp.float32 if kept else jnp.bfloat16),
        compiler_params=params(),
        name="slope_kept" if kept else "slope_sent",
    )(pre, low, weight)


def small_body(kept, got, got_two, ids, bias, send, keep, square, lines):
    f32 = jnp.float32
    core = lax.axis_index("client_2")
    sums = kept[1] + got[1].astype(f32) + got_two[...].astype(f32)
    width = sums.shape[1]
    across = width // LANES
    clients = ids.shape[1]
    count = 2 * send.shape[0]
    mine = sums[:clients]
    square[...] = jnp.full(square.shape, jnp.sum(mine * mine))
    line = lax.broadcasted_iota(jnp.int32, (count * clients, clients), 0)
    which = line // clients
    side = jnp.where(which < len(ALL), 1 - core, core)
    target = owner_at(side, which & 3, (which >> 2) & 3) * clients + line % clients
    selector = jnp.where(target == ids[...], 1.0, 0.0).astype(jnp.bfloat16)
    placed = jnp.dot(selector, mine.astype(jnp.bfloat16), preferred_element_type=f32)
    spans = sums[clients:]
    lines[...] = jnp.zeros(lines.shape, f32)
    for r in range(SPANS // 8):
        for c in range(across):
            lines[r * across + c] = spans[8 * r : 8 * r + 8, c * LANES : (c + 1) * LANES]
    bias_row = jnp.sum(bias[...], axis=0, keepdims=True)
    for c in range(across):
        lines[SPANS // 8 * across, c : c + 1, :] = bias_row[:, c * LANES : (c + 1) * LANES]
    groups = clients // 8
    share = send.shape[1] - groups * across
    for k in range(count):
        out = send if k < len(ALL) else keep
        at = k % len(ALL)
        for g in range(groups):
            for c in range(across):
                top = k * clients + 8 * g
                block = placed[top : top + 8, c * LANES : (c + 1) * LANES]
                out[at, g * across + c] = block.astype(out.dtype)
        owner = owner_at(1 - core if k < len(ALL) else core, *ALL[at])
        out[at, groups * across :] = lines[pl.ds(share * owner, share)].astype(out.dtype)


def small_sends(kept, got, got_two, ids, bias, share):
    width = kept.shape[2]
    tiles = ids.shape[1] // 8 * (width // LANES) + share
    shape = (len(ALL), tiles, 8, LANES)
    return pl.pallas_call(
        small_body,
        in_specs=[whole()] * 5,
        out_specs=[whole()] * 3,
        out_shape=[
            jax.ShapeDtypeStruct(shape, jnp.bfloat16),
            jax.ShapeDtypeStruct(shape, jnp.float32),
            jax.ShapeDtypeStruct((8, LANES), jnp.float32),
        ],
        scratch_shapes=[pltpu.VMEM((2 * len(ALL) * share, 8, LANES), jnp.float32)],
        compiler_params=pltpu.CompilerParams(vmem_limit_bytes=LIMIT),
        name="small_sends",
    )(kept, got, got_two, ids, bias)


def core_sum_body(keep, arrived, own, one, two, three):
    total = keep[...] + arrived[...].astype(jnp.float32)
    own[...] = total[0:4]
    for k, out in ((1, one), (2, two), (3, three)):
        out[...] = total[4 * k : 4 * k + 4].astype(out.dtype)


def core_sum(keep, arrived):
    shape = (keep.shape[0] // 4, *keep.shape[1:])
    low = jax.ShapeDtypeStruct(shape, jnp.bfloat16)
    return simple_call(core_sum_body, (keep, arrived), [jax.ShapeDtypeStruct(shape, jnp.float32), low, low, low])


def line_sum_body(own, side_one, side_two, side_three, mine, one, two, three):
    f32 = jnp.float32
    total = own[...] + side_one[...].astype(f32) + side_two[...].astype(f32) + side_three[...].astype(f32)
    mine[...] = total[0]
    for k, out in ((1, one), (2, two), (3, three)):
        out[...] = total[k].astype(out.dtype)


def line_sum(own, arrived):
    shape = own.shape[1:]
    low = jax.ShapeDtypeStruct(shape, jnp.bfloat16)
    return simple_call(line_sum_body, (own, *arrived), [jax.ShapeDtypeStruct(shape, jnp.float32), low, low, low])


def join_body(keep, got_a, got_b, head, one, two, three):
    for k, out in enumerate((head, one, two, three)):
        side = got_a if k < 2 else got_b
        out[...] = (keep[k] + side[k % 2].astype(jnp.float32)).astype(out.dtype)


def join(keep, got_a, got_b):
    low = jax.ShapeDtypeStruct(keep.shape[1:], jnp.bfloat16)
    own = jax.ShapeDtypeStruct(keep.shape[1:], jnp.float32)
    return simple_call(join_body, (keep, got_a, got_b), [own, low, low, low])


def close_body(head, one, two, three, small, s_one, s_two, s_three, square, total, embed, message):
    f32 = jnp.float32
    width = head.shape[0]
    lines = small.shape[0]
    across = width // LANES
    peers, share = message.shape[0], message.shape[1] - 1
    rows = lines - share
    part = jnp.zeros((8, LANES), f32)
    for t in range(lines):
        tile = small[t] + s_one[t].astype(f32) + s_two[t].astype(f32) + s_three[t].astype(f32)
        if t < rows:
            r, c = divmod(t, across)
            embed[8 * r : 8 * r + 8, c * LANES : (c + 1) * LANES] = tile
        else:
            low = tile.astype(message.dtype)
            part = part + low.astype(f32) * low.astype(f32)
            for p in range(peers):
                message[p, t - rows] = low
    value = head[...]
    for side in (one, two, three):
        value = value + side[...].astype(f32)
    total[...] = value
    column = lax.broadcasted_iota(jnp.int32, (8, LANES), 1)
    line = lax.broadcasted_iota(jnp.int32, (8, LANES), 0)
    sums = jnp.where(column == 1, square[...], jnp.sum(part))
    sums = jnp.where(column == 0, jnp.sum(value * value), sums)
    coarse = sums.astype(message.dtype).astype(f32)
    scalars = jnp.where(line == 0, coarse, jnp.where(line == 1, sums - coarse, 0.0)).astype(message.dtype)
    for p in range(peers):
        message[p, share] = scalars


def close(head, arrived, small, small_arrived, square, peers, share):
    width = head.shape[0]
    rows = 8 * (small.shape[0] - share) * LANES // width
    return simple_call(
        close_body,
        (head, *arrived, small, *small_arrived, square),
        [
            jax.ShapeDtypeStruct((width, LANES), jnp.float32),
            jax.ShapeDtypeStruct((rows, width), jnp.float32),
            jax.ShapeDtypeStruct((peers, share + 1, 8, LANES), jnp.bfloat16),
        ],
    )


def turn_body(value, out):
    out[...] = value[...].T


def turn(value):
    return simple_call(turn_body, (value,), [jax.ShapeDtypeStruct(value.shape[::-1], value.dtype)])[0]


def subtotal_body(arrived, out):
    last = arrived.shape[1] - 1
    total = None
    for p in range(arrived.shape[0]):
        some = arrived[p, last].astype(jnp.float32)
        total = some if total is None else total + some
    out[...] = jnp.sum(total, axis=0, keepdims=True)


def subtotal(arrived):
    shape = jax.ShapeDtypeStruct((1, arrived.shape[3]), jnp.float32)
    return simple_call(subtotal_body, (arrived,), [shape])[0]


def scale_body(counts, mine, one, two, three, head, embed, shares, head_grad, bias_grad, embed_grad, span_grad):
    f32 = jnp.float32
    totals = (mine[...] + two[...]) + (one[...] + three[...])

    def factor(k):
        mean = totals[:, k : k + 1] / counts[k] + EPSILON
        return jnp.minimum(1.0, 1.0 / jnp.sqrt(mean))

    head_grad[...] = factor(0) * head[...]
    embed_grad[...] = factor(1) * embed[...]
    rest = factor(2)
    across = span_grad.shape[1] // LANES
    share = shares.shape[1] - 1
    for t in range(SPANS // 8 * across):
        r, c = divmod(t, across)
        tile = shares[t // share, t % share].astype(f32)
        span_grad[8 * r : 8 * r + 8, c * LANES : (c + 1) * LANES] = rest * tile
    t = SPANS // 8 * across
    bias_grad[...] = rest * shares[t // share, t % share].astype(f32)


def scale(counts, squares, head, embed, shares):
    width = head.shape[1]
    return simple_call(
        lambda *refs: scale_body(counts, *refs),
        (*squares, head, embed, shares),
        [
            jax.ShapeDtypeStruct(head.shape, jnp.float32),
            jax.ShapeDtypeStruct((width // LANES, LANES), jnp.float32),
            jax.ShapeDtypeStruct(embed.shape, jnp.float32),
            jax.ShapeDtypeStruct((SPANS, width), jnp.float32),
        ],
    )


def flipped(first, second):
    pairs = []
    for z in range(4):
        for x in range(4):
            pairs.append(((z * 4 + x) * 2, ((z ^ first[0]) * 4 + (x ^ first[1])) * 2))
            pairs.append(((z * 4 + x) * 2 + 1, ((z ^ second[0]) * 4 + (x ^ second[1])) * 2 + 1))
    return pairs


def along_u(x, k):
    return lax.ppermute(x, CLIENT, flipped((0, k), (k, 0)))


def along_v(x, k):
    return lax.ppermute(x, CLIENT, flipped((k, 0), (0, k)))


def to_core(x):
    return lax.ppermute(x, "client_2", [(0, 1), (1, 0)])


def along_head(x, low, high):
    axes = ("client_2", "head")
    pairs = [(h, h ^ low) for h in range(4)] + [(4 + h, 4 + (h ^ high)) for h in range(4)]
    return lax.ppermute(x, axes, pairs)


def wide(x):
    return x.astype(jnp.float32)


def narrow(x):
    return x.astype(jnp.bfloat16)


def to_head(x, k):
    return lax.ppermute(x, "head", [(h, h ^ k) for h in range(4)])


def around(move, one, two, three):
    two = move(two, 2)
    one = move(one, 1)
    three = move(three, 3)
    return one, two, three


def exchange(x, axes):
    return lax.all_to_all(x, axes, 0, 0, tiled=True)


def per_device(pre, delta, head_weight, client_ids):
    hidden_width = pre.shape[1]
    emit_here = delta.shape[1]
    clients_here = client_ids.shape[0]
    head_devices = lax.axis_size("head")
    peers = lax.axis_size(CLIENT)
    share = -(-(SPANS // 8 * (emit_here // LANES) + 1) // peers)

    low, turned, bias_part, early = prepare(delta, pre)
    part = partner_call(lambda: range(len(FIRST)), early, turned)
    arrived_first = to_core(part)
    part = partner_call(partner_kept, pre, turned)
    arrived_kept = to_core(part)
    near, far = first_call(pre, turned, arrived_first)
    near = along_u(near, 1)
    far = along_u(far, 3)
    sent = slope_call(False, pre, low, head_weight)
    got = along_head(sent, 1, 3)
    kept = slope_call(True, pre, low, head_weight)
    message = narrow(kept[0] + wide(got[0]))
    got_two = along_head(message, 3, 1)
    send_a, send_b, keep = kept_call(pre, turned, arrived_kept, near, far)
    got_a = along_u(send_a, 3)
    got_b = along_u(send_b, 1)
    small_send, small_keep, embed_square = small_sends(kept, got, got_two, client_ids[None, :], bias_part, share)
    small_got = to_core(small_send)
    own, one, two, three = core_sum(small_keep, small_got)
    small_arrived = around(along_v, one, two, three)
    final, one, two, three = join(keep, got_a, got_b)
    arrived = around(along_v, one, two, three)
    small, one, two, three = line_sum(own, small_arrived)
    small_arrived = around(along_u, one, two, three)
    total, embed_raw, message = close(final, arrived, small, small_arrived, embed_square, peers, share)
    shares = exchange(message, CLIENT)
    head_raw = turn(total)
    squares = subtotal(shares)
    squares = (squares, *around(to_head, squares, squares, squares))
    emit_total = emit_here * head_devices
    counts = (
        float(hidden_width * emit_total),
        float(clients_here * peers * hidden_width),
        float(SPANS * hidden_width + emit_total),
    )
    head_grad, bias_grad, embed_grad, span_grad = scale(counts, squares, head_raw, embed_raw, shares)
    return head_grad, bias_grad.reshape(emit_here), embed_grad, span_grad


def solution(mesh):
    torus = Mesh(
        mesh.devices.reshape(4, 4, 2, mesh.shape["head"]),
        ("client_0", "client_1", "client_2", "head"),
    )
    return jax.shard_map(
        per_device,
        mesh=torus,
        in_specs=(P(CLIENT, None), P(CLIENT, "head"), P(None, "head"), P(CLIENT)),
        out_specs=(P(CLIENT, "head"), P("head"), P(CLIENT, "head"), P(None, "head")),
        check_vma=False,
    )
```
